32 devices in a mesh: group: 2 (over y), expert: 4 (over z), tensor: 2 (over x), seq: 2 (over core).
Axes of the slice: x: 2, y: 2, z: 4, core: 2. Of those that a mesh axis runs over, the one named last changes fastest.
Arguments:
- queries: bfloat16 [2048, 2048], P(('group', 'expert', 'seq'), 'tensor'), parts along dimension 0, may hold values from -6 to 6
- keys_values: bfloat16 [2048, 4, 128], P(('group', 'expert', 'seq'), 'tensor'), parts along dimension 0, may hold values from -6 to 6
- residual: bfloat16 [2048, 1440], P(('group', 'expert', 'seq')), parts along dimension 0, may hold values from -6 to 6
- sink_logits: float32 [32], P('tensor'), may hold values from 0 to 6
- norm_gain: float32 [1440], replicated, may hold values from 0.5 to 1.5
- out_proj: bfloat16 [2048, 1440], P('tensor', 'seq'), may hold values from -0.125 to 0.125
- shared_gate_up: bfloat16 [1440, 2, 512], P('seq', None, 'tensor'), may hold values from -0.15625 to 0.15625
- shared_down: bfloat16 [512, 1440], P('tensor', 'seq'), may hold values from -0.25 to 0.25
- expert_gate_up: bfloat16 [8, 1440, 2, 1440], P(('expert', 'seq'), None, None, 'tensor'), may hold values from -0.15625 to 0.15625
- expert_down: bfloat16 [8, 1440, 1440], P(('expert', 'seq'), 'tensor'), may hold values from -0.15625 to 0.15625
- expert_ids: int32 [2048, 4], P(('group', 'expert', 'seq')), parts along dimension 0, may hold values from 0 to 7, all different within a row; in each aligned block of 128 rows (0 to 127, 128 to 255, ...) at most 96 rows name the same one
- gate_weights: float32 [2048, 4], P(('group', 'expert', 'seq')), parts along dimension 0, may hold values from 0.1 to 1
Outputs:
- mixed: bfloat16 [2048, 1440], P(('group', 'expert', 'seq'), 'tensor'), parts along dimension 0
The draws below stay inside these ranges and needn't reach their ends.
There are 2 independent parts, one for each index of `group`. The reference program is written for one: setup_inputs(seed, part) draws one part's arguments, and reference() takes and returns one part's arrays. A program takes and returns all parts, laid end to end along the dimension named above; an argument that names none is the same for every part. Nothing has to cross between parts.
Inputs may be any that keep to these rules, and one draw needn't show every extreme that they name: `expert_ids`: in each aligned block of 128 tokens (the tokens of one device), no expert is named by more than 96 tokens; the 4 ids of a token differ.
All inputs are finite; a program needn't handle non-finite values.
Results may differ from the reference program's by a relative error of at most 0.014.
Values may be sent and summed in bfloat16 or wider, within the bound.
A program may use at most 64 MiB of HBM per device.

```python
import math
import jax
import jax.numpy as jnp
import numpy as np
from jax import lax

D = 1440
HEADS = 32
KV_HEADS = 4
HEAD_DIM = 64
WINDOW = 128
FF = 1440
SHARED_FF = 512
TOP = 4
TOK_DEV = 128
EXPERTS = 8
TOKENS = 1024
CAP = 96
N_TENSOR = 2


def base_values(key, shape):
    return jnp.clip(jax.random.normal(key, shape, jnp.float32), -5.0, 5.0)


def draw_queries(key, part):
    values = base_values(jax.random.fold_in(key, 1), (TOKENS, HEADS * HEAD_DIM))
    return values.astype(jnp.bfloat16)


def draw_keys_values(key, part):
    key_part = base_values(jax.random.fold_in(key, 2), (TOKENS, KV_HEADS, HEAD_DIM))
    value_part = base_values(jax.random.fold_in(key, 3), (TOKENS, KV_HEADS, HEAD_DIM))
    return jnp.concatenate([key_part, value_part], axis=-1).astype(jnp.bfloat16)


def block_scale(own_key, extent, cuts, low, top_value):
    level = 1.0
    for dim, blocks in cuts:
        draws = jax.random.uniform(jax.random.fold_in(jax.random.fold_in(own_key, 6), dim), (blocks,), jnp.float32, low / len(cuts), top_value / len(cuts))
        level = level * jnp.repeat(jnp.exp(draws), extent[dim] // blocks).reshape((-1,) + (1,) * (len(extent) - 1 - dim))
    return level


def deal_out(stream_key, own, number, rows, number_of, top, bound, slope):
    ranking = jax.random.permutation(stream_key, number_of)
    packed, usual = shares(number_of, rows * top, bound, slope, True), shares(number_of, rows * top, bound, slope, False)
    places = jnp.arange(number_of)

    def named(tallies, rotation):
        used = int((tallies > 0).sum())
        fixed = max(1, used // 4)
        moved = fixed + (places - fixed + rotation * (used - fixed)) % max(1, number_of - fixed)
        return jnp.zeros((number_of,), jnp.int32).at[ranking[jnp.where(places < fixed, places, moved)]].set(jnp.asarray(tallies, jnp.int32))

    tallies = jnp.where(number % 4 == 0, named(packed, number // 4), named(usual, number - number // 4 - 1))
    mixed = jax.random.permutation(jax.random.fold_in(own, 3), number_of)
    donor, taker = mixed[0:number_of // 2 * 2:2], mixed[1:number_of // 2 * 2:2]
    room = jnp.minimum(tallies[donor] - 1, bound - tallies[taker]) // 2
    room = jnp.where((donor == ranking[0]) | (taker == ranking[0]) | (tallies[taker] == 0), 0, jnp.maximum(room, 0))
    moved = jax.random.randint(jax.random.fold_in(own, 4), (number_of // 2,), 0, 1 << 20) % (room + 1)
    tallies = tallies.at[donor].add(-moved).at[taker].add(moved)
    members = jnp.searchsorted(jnp.cumsum(tallies), jnp.arange(rows * top), side="right").astype(jnp.int32)
    table = members.reshape(top, rows).T
    table = table[jax.random.permutation(jax.random.fold_in(own, 1), rows)]
    rotation = jax.random.randint(jax.random.fold_in(own, 2), (rows, 1), 0, top)
    return jnp.take_along_axis(table, (jnp.arange(top)[None, :] + rotation) % top, axis=1)


def shares(number_of, total, reach, lean, full):
    weights = [(1 << 20) // math.isqrt(standing ** lean) + 1 for standing in range(1, number_of + 1)]
    largest = reach if full else min(reach, max(-(-total // number_of), total * weights[0] // sum(weights)))
    least = 1 if total - largest >= number_of - 1 else 0
    counts, surplus = [largest] + [least] * (number_of - 1), total - largest - least * (number_of - 1)
    while surplus > 0:
        candidates = [i for i in range(1, number_of) if counts[i] < largest] or [i for i in range(1, number_of) if counts[i] < reach]
        whole, left = sum([weights[i] for i in candidates]), surplus
        for i in candidates:
            extra = min(reach - counts[i], max(1, left * weights[i] // whole), surplus)
            counts[i] = counts[i] + extra
            surplus = surplus - extra
    return np.array(counts)


def centred(own_key, extent, deviation, bound, pieces=(), kind=jnp.bfloat16):
    array = deviation * jax.random.normal(own_key, extent, jnp.float32)
    if pieces:
        array = array * block_scale(own_key, extent, pieces, -0.22, 0.18)
    return jnp.clip(array, -bound, bound).astype(kind)


def setup_inputs(seed: int = 0, part: int = 0) -> dict:
    key_of = jax.random.split(jax.random.key(seed), 13)
    part_keys = jax.random.split(jax.random.fold_in(key_of[12], part), 13)
    queries = draw_queries(jax.random.fold_in(jax.random.fold_in(key_of[12], part), 71), part)
    keys_values = draw_keys_values(jax.random.fold_in(jax.random.fold_in(key_of[12], part), 71), part)
    residual = centred(part_keys[2], (TOKENS, D), 1.0, 6.0, ((0, 8),))
    sink_logits = jnp.clip(6.0 * jax.random.uniform(key_of[3], (HEADS,), jnp.float32) ** block_scale(key_of[3], (HEADS,), ((0, 2),), -0.2, 0.2), 0.0, 6.0)
    norm_gain = jnp.clip(1.0 + 0.1 * jax.random.normal(key_of[4], (D,), jnp.float32), 0.5, 1.5)
    out_proj = centred(key_of[5], (HEADS * HEAD_DIM, D), (HEADS * HEAD_DIM) ** -0.5, 0.125, ((0, 2), (1, 2)))
    shared_gate_up = centred(key_of[6], (D, 2, SHARED_FF), D ** -0.5, 0.15625, ((0, 2), (2, 2)))
    shared_down = centred(key_of[7], (SHARED_FF, D), SHARED_FF ** -0.5, 0.25, ((0, 2), (1, 2)))
    expert_gate_up = centred(key_of[8], (EXPERTS, D, 2, FF), D ** -0.5, 0.15625, ((0, 8), (3, 2)))
    expert_down = centred(key_of[9], (EXPERTS, FF, D), FF ** -0.5, 0.15625, ((0, 8), (1, 2)))
    expert_ids_keys = jax.random.split(jax.random.fold_in(part_keys[10], 1), TOKENS // TOK_DEV)
    expert_ids_turns = jax.random.permutation(jax.random.fold_in(part_keys[10], 3), TOKENS // TOK_DEV)
    expert_ids = jax.vmap(lambda own, number: deal_out(jax.random.fold_in(part_keys[10], 2), own, number, TOK_DEV, EXPERTS, TOP, CAP, 0))(expert_ids_keys, expert_ids_turns).reshape((TOKENS, TOP))
    gate_weights = jnp.clip(0.1 + 0.9 * jax.random.uniform(part_keys[11], (TOKENS, TOP), jnp.float32) ** block_scale(part_keys[11], (TOKENS, TOP), ((0, 8),), -0.2, 0.2), 0.1, 1.0)
    return dict(queries=queries, keys_values=keys_values, residual=residual, sink_logits=sink_logits, norm_gain=norm_gain, out_proj=out_proj, shared_gate_up=shared_gate_up, shared_down=shared_down, expert_gate_up=expert_gate_up, expert_down=expert_down, expert_ids=expert_ids, gate_weights=gate_weights)


norm_eps = 1e-05
glu_alpha = 1.702

def glu_act(gate_pre, up_pre):
    return (up_pre + 1.0) * gate_pre * jax.nn.sigmoid(glu_alpha * gate_pre)

def attend_block(query_block, pair_block, sink_logits, block_index):
    count_rows = query_block.shape[0]
    kv_count = pair_block.shape[1]
    head_size = pair_block.shape[2] // 2
    group_size = query_block.shape[1] // (head_size * kv_count)
    grouped = query_block.reshape(count_rows, kv_count, group_size, head_size).astype(jnp.float32)
    key_part = pair_block[:, :, :head_size].astype(jnp.float32)
    value_part = pair_block[:, :, head_size:].astype(jnp.float32)
    scores = jnp.einsum('pkgd,jkd->kgpj', grouped, key_part) / math.sqrt(head_size)
    query_pos = jnp.arange(count_rows, dtype=jnp.int32)[:, None]
    key_rel = jnp.arange(2 * count_rows, dtype=jnp.int32)[None, :] - count_rows
    distance = query_pos - key_rel
    visible = (distance >= 0) & (distance < WINDOW) & (block_index * count_rows + key_rel >= 0)
    scores = jnp.where(visible[None, None], scores, -jnp.inf)
    sink_term = sink_logits.reshape(kv_count, group_size)[:, :, None, None].astype(jnp.float32)
    top_score = jnp.maximum(lax.optimization_barrier(jnp.max(scores, axis=-1, keepdims=True)), sink_term)
    expo = jnp.exp(scores - top_score)
    denom = lax.optimization_barrier(jnp.sum(expo, axis=-1, keepdims=True)) + jnp.exp(sink_term - top_score)
    attn_weights = (expo / denom).astype(jnp.bfloat16)
    context = jnp.einsum('kgpj,jkd->pkgd', attn_weights.astype(jnp.float32), value_part)
    return context.astype(jnp.bfloat16).reshape(count_rows, kv_count * group_size * head_size)

def sliced_down(hidden, down_weight, slices):
    piece_width = hidden.shape[1] // slices
    total = jnp.zeros((hidden.shape[0], down_weight.shape[1]), jnp.float32)
    for slice_index in range(slices):
        part_sum = jnp.dot(hidden[:, slice_index * piece_width:(slice_index + 1) * piece_width], down_weight[slice_index * piece_width:(slice_index + 1) * piece_width], preferred_element_type=jnp.float32)
        rounded = lax.optimization_barrier(part_sum.astype(jnp.bfloat16))
        total = total + rounded.astype(jnp.float32)
    return total

def reference(queries, keys_values, residual, sink_logits, norm_gain, out_proj, shared_gate_up, shared_down, expert_gate_up, expert_down, expert_ids, gate_weights):
    block_count = TOKENS // TOK_DEV
    padded_pairs = jnp.concatenate([jnp.zeros((TOK_DEV,) + keys_values.shape[1:], keys_values.dtype), keys_values], axis=0)

    def one_block(block_index):
        start = (block_index * TOK_DEV).astype(jnp.int32)
        query_block = lax.dynamic_slice_in_dim(queries, start, TOK_DEV, 0)
        pair_block = lax.dynamic_slice_in_dim(padded_pairs, start, 2 * TOK_DEV, 0)
        return attend_block(query_block, pair_block, sink_logits, block_index)
    context = lax.map(one_block, jnp.arange(block_count, dtype=jnp.int32)).reshape(TOKENS, HEADS * HEAD_DIM)
    attn = jnp.dot(context, out_proj, preferred_element_type=jnp.float32)
    stream = residual.astype(jnp.float32) + attn
    scale = lax.rsqrt(lax.optimization_barrier(jnp.mean(stream * stream, axis=-1, keepdims=True)) + norm_eps)
    normed = (stream * scale * norm_gain.astype(jnp.float32)).astype(jnp.bfloat16)
    shared_pre = jnp.einsum('pd,dcf->pcf', normed.astype(jnp.float32), shared_gate_up.astype(jnp.float32))
    shared_hidden = glu_act(shared_pre[:, 0], shared_pre[:, 1]).astype(jnp.bfloat16)
    shared_out = sliced_down(shared_hidden, shared_down, N_TENSOR)
    limit = block_count * CAP
    flat_ids = expert_ids.reshape(-1)
    flat_gates = jnp.concatenate([gate_weights.reshape(-1), jnp.zeros((1,), jnp.float32)])
    normed_padded = jnp.concatenate([normed, jnp.zeros((1, D), jnp.bfloat16)], axis=0)

    def one_expert(routed_acc, expert):
        chosen = jnp.nonzero(flat_ids == expert, size=limit, fill_value=TOKENS * TOP)[0].astype(jnp.int32)
        token_index = chosen // TOP
        rows_in = normed_padded[token_index]
        gate_up = lax.dynamic_index_in_dim(expert_gate_up, expert, 0, keepdims=False)
        down_weight = lax.dynamic_index_in_dim(expert_down, expert, 0, keepdims=False)
        expert_pre = jnp.einsum('nd,dcf->ncf', rows_in.astype(jnp.float32), gate_up.astype(jnp.float32))
        expert_hidden = glu_act(expert_pre[:, 0], expert_pre[:, 1]).astype(jnp.bfloat16)
        expert_out = sliced_down(expert_hidden, down_weight, N_TENSOR)
        weighted = expert_out * flat_gates[chosen][:, None]
        return (routed_acc.at[token_index].add(weighted), None)
    routed_acc, _ = lax.scan(one_expert, jnp.zeros((TOKENS + 1, D), jnp.float32), jnp.arange(EXPERTS, dtype=jnp.int32))
    routed = routed_acc[:TOKENS]
    return (stream + shared_out + routed).astype(jnp.bfloat16)
```

```python
import functools
import math

import jax
import jax.numpy as jnp
from jax import lax
from jax.experimental import pallas as pl
from jax.experimental.pallas import tpu as pltpu
from jax.sharding import PartitionSpec as P

WINDOW = 128


norm_eps = 1e-05
glu_alpha = 1.702


def shifted(value, axis, steps):
    count = lax.axis_size(axis)
    initial, last = (max(0, -steps), min(count, count - steps))
    return lax.ppermute(value, axis, [(source, source + steps) for source in range(initial, last)])


def glu_act(gate_pre, up_pre):
    return (up_pre + 1.0) * gate_pre * jax.nn.sigmoid(glu_alpha * gate_pre)


def attend_local(queries, keys_values, sink_logits, block_index):
    count_rows = queries.shape[0]
    kv_count = keys_values.shape[1]
    head_size = keys_values.shape[2] // 2
    group_size = queries.shape[1] // (head_size * kv_count)
    earlier = shifted(keys_values, ("expert", "seq"), 1)
    pair_block = jnp.concatenate([earlier, keys_values], axis=0)
    grouped = queries.reshape(count_rows, kv_count, group_size, head_size)
    key_part = pair_block[:, :, :head_size]
    value_part = pair_block[:, :, head_size:]
    scores = jnp.einsum(
        "pkgd,jkd->kgpj", grouped, key_part, preferred_element_type=jnp.float32
    ) / math.sqrt(head_size)
    query_pos = jnp.arange(count_rows, dtype=jnp.int32)[:, None]
    key_rel = jnp.arange(2 * count_rows, dtype=jnp.int32)[None, :] - count_rows
    distance = query_pos - key_rel
    visible = (distance >= 0) & (distance < WINDOW) & (block_index * count_rows + key_rel >= 0)
    scores = jnp.where(visible[None, None], scores, -jnp.inf)
    sink_term = sink_logits.reshape(kv_count, group_size)[:, :, None, None]
    top_score = jnp.maximum(jnp.max(scores, axis=-1, keepdims=True), sink_term)
    expo = jnp.exp(scores - top_score)
    denom = jnp.sum(expo, axis=-1, keepdims=True) + jnp.exp(sink_term - top_score)
    attn_weights = (expo / denom).astype(jnp.bfloat16)
    context = jnp.einsum(
        "kgpj,jkd->pkgd", attn_weights, value_part, preferred_element_type=jnp.float32
    )
    return context.astype(jnp.bfloat16).reshape(count_rows, kv_count * group_size * head_size)


def local(
    queries,
    keys_values,
    residual,
    sink_logits,
    norm_gain,
    out_proj,
    shared_gate_up,
    shared_down,
    expert_gate_up,
    expert_down,
    expert_ids,
    gate_weights,
):
    block_index = lax.axis_index(("expert", "seq"))
    context = attend_local(queries, keys_values, sink_logits, block_index)
    proj_full, shared_gu_full, shared_dn_full = (
        lax.all_gather(out_proj, "seq", axis=1, tiled=True),
        lax.all_gather(shared_gate_up, "seq", axis=0, tiled=True),
        lax.all_gather(shared_down, "seq", axis=1, tiled=True),
    )
    attn_part = jnp.dot(context, proj_full, preferred_element_type=jnp.float32)
    attn = lax.psum(attn_part.astype(jnp.bfloat16), "tensor").astype(jnp.float32)
    stream = residual.astype(jnp.float32) + attn
    scale = lax.rsqrt(jnp.mean(stream * stream, axis=-1, keepdims=True) + norm_eps)
    normed = (stream * scale * norm_gain).astype(jnp.bfloat16)
    shared_pre = jnp.einsum(
        "pd,dcf->pcf", normed, shared_gu_full, preferred_element_type=jnp.float32
    )
    shared_hidden = glu_act(shared_pre[:, 0], shared_pre[:, 1]).astype(jnp.bfloat16)
    shared_part = jnp.dot(shared_hidden, shared_dn_full, preferred_element_type=jnp.float32)
    count_rows = normed.shape[0]
    width = normed.shape[1]
    top_count = expert_ids.shape[1]
    expert_count = expert_gate_up.shape[0] * lax.axis_size(("expert", "seq"))
    capacity = max(2, 3 * count_rows * top_count // (2 * expert_count))
    tensor_size = lax.axis_size("tensor")
    col_width = width // tensor_size
    col_start = lax.axis_index("tensor") * col_width
    flat_ids = expert_ids.reshape(-1)
    assign_count = count_rows * top_count
    onehot = (flat_ids[:, None] == jnp.arange(expert_count, dtype=jnp.int32)[None, :]).astype(
        jnp.int32
    )
    ranks = jnp.sum((jnp.cumsum(onehot, axis=0) - 1) * onehot, axis=1)
    slots = flat_ids * capacity + ranks
    slot_source = (
        jnp.full((expert_count * capacity,), assign_count, jnp.int32)
        .at[slots]
        .set(jnp.arange(assign_count, dtype=jnp.int32))
    )
    token_of_slot = jnp.where(slot_source < assign_count, slot_source // top_count, count_rows)
    normed_padded = jnp.concatenate([normed, jnp.zeros((1, width), jnp.bfloat16)], axis=0)
    outgoing = normed_padded[token_of_slot].reshape(expert_count, capacity, width)
    arrived = lax.all_to_all(outgoing, ("expert", "seq"), split_axis=0, concat_axis=0, tiled=True)
    expert_pre = jnp.einsum(
        "scd,dhf->schf", arrived, expert_gate_up[0], preferred_element_type=jnp.float32
    )
    expert_hidden = glu_act(expert_pre[:, :, 0], expert_pre[:, :, 1]).astype(jnp.bfloat16)
    expert_part = jnp.einsum(
        "scf,fd->scd", expert_hidden, expert_down[0], preferred_element_type=jnp.float32
    )
    returned = lax.all_to_all(
        expert_part.astype(jnp.bfloat16), ("expert", "seq"), split_axis=0, concat_axis=0, tiled=True
    )
    picked = (
        returned.reshape(expert_count * capacity, width)[slots]
        .astype(jnp.float32)
        .reshape(count_rows, top_count, width)
    )
    routed = jnp.sum(picked * gate_weights[:, :, None], axis=1)
    shared_rounded = lax.optimization_barrier(shared_part.astype(jnp.bfloat16))
    combined = shared_rounded.astype(jnp.float32) + routed
    summed = lax.psum_scatter(
        combined.astype(jnp.bfloat16), "tensor", scatter_dimension=1, tiled=True
    ).astype(jnp.float32)
    stream_cols = lax.dynamic_slice_in_dim(stream, col_start, col_width, 1)
    return (stream_cols + summed).astype(jnp.bfloat16)


MESH_ID = pl.DeviceIdType.MESH
LANES = 128


def pad_lanes(count):
    return -(-count // LANES) * LANES


def at_table(table, index):
    value = jnp.int32(table[0])
    for place in range(1, len(table)):
        value = jnp.where(index == place, jnp.int32(table[place]), value)
    return value


def when(condition, action):
    pl.when(condition)(action)


def greet(others):
    barrier = pltpu.get_barrier_semaphore()
    for condition, device in others:
        def send(device=device):
            pl.semaphore_signal(barrier, inc=1, device_id=device, device_id_type=MESH_ID)
        send() if condition is None else when(condition, send)
    count = sum(jnp.int32(1) if condition is None else condition.astype(jnp.int32) for condition, _ in others)
    pl.semaphore_wait(barrier, count)


def remote(source, target, send_sem, recv_sem, device):
    return pltpu.make_async_remote_copy(
        src_ref=source, dst_ref=target, send_sem=send_sem, recv_sem=recv_sem,
        device_id=device, device_id_type=MESH_ID,
    )


def front_kernel(
    chips, q_ref, kv_ref, res_ref, sink_ref, gain_ref, proj_ref, sgu_ref, sdn_ref, ids_ref, gw_ref,
    nbuf, stream_ref, sgu_out, sdn_out,
    kv_prev, proj_other, ctx, part, xsend, xrecv,
    wsend, wrecv, kvsem, xsem, gsend, grecv,
):
    e, s, t = lax.axis_index("expert"), lax.axis_index("seq"), lax.axis_index("tensor")
    rows = q_ref.shape[0]
    half_rows = rows // 2
    col = proj_ref.shape[1]
    depth = sgu_ref.shape[0]
    width = 2 * col
    core, across = {"seq": 1 - s}, {"tensor": 1 - t}
    up, down = {"expert": e + 1}, {"expert": e - 1}
    has_up, has_down = e < chips - 1, e > 0
    greet([
        (None, core), (None, across), (has_up, up), (has_down, down),
        ((s == 1) & has_up, {"expert": e + 1, "seq": 0}),
        ((s == 0) & has_down, {"expert": e - 1, "seq": 1}),
    ])
    first = (e == 0) & (s == 0)
    kv_near = remote(kv_ref, kv_prev, kvsem.at[0], kvsem.at[1], core)
    kv_far = remote(kv_ref, kv_prev, kvsem.at[0], kvsem.at[1], {"expert": e + 1, "seq": 0})
    when(s == 0, lambda: kv_near.start())
    when((s == 1) & has_up, lambda: kv_far.start())
    weights = [
        remote(proj_ref, proj_other, wsend.at[0], wrecv.at[0], core),
        remote(sgu_ref, sgu_out.at[pl.ds(s * depth, depth)], wsend.at[1], wrecv.at[1], core),
        remote(sdn_ref, sdn_out.at[s], wsend.at[2], wrecv.at[2], core),
    ]
    for copy in weights:
        copy.start()
    sgu_out[pl.ds(s * depth, depth), :] = sgu_ref[...]
    sdn_out[s] = sdn_ref[...]

    def blank():
        kv_prev[...] = jnp.zeros_like(kv_prev)
    when(first, blank)
    when(jnp.logical_not(first), lambda: kv_near.wait_recv())

    lane = lax.broadcasted_iota(jnp.int32, (rows, LANES), 1)
    head = LANES // 2
    low = lane < head
    own_mask = lax.broadcasted_iota(jnp.int32, (rows, rows), 1) <= lax.broadcasted_iota(jnp.int32, (rows, rows), 0)
    bias = jnp.where(first, -1e30, 0.0).astype(jnp.float32)
    kv_count = kv_ref.shape[1] // LANES
    pairs = q_ref.shape[1] // LANES // kv_count
    inv = 1.0 / math.sqrt(head)

    def halves(ref, group):
        value = ref[:, group * LANES:(group + 1) * LANES].astype(jnp.float32)
        turned = pltpu.roll(value, head, 1)
        zero = jnp.zeros_like(value)
        return [
            jnp.where(low, value, zero).astype(jnp.bfloat16), jnp.where(low, zero, turned).astype(jnp.bfloat16),
            jnp.where(low, turned, zero).astype(jnp.bfloat16), jnp.where(low, zero, value).astype(jnp.bfloat16),
        ]

    for group in range(kv_count):
        mine, before = halves(kv_ref, group), halves(kv_prev, group)
        keys = jnp.concatenate([mine[0], before[0], mine[1], before[1]], axis=0)
        values = jnp.concatenate([mine[2], before[2], mine[3], before[3]], axis=0)
        for pair in range(pairs):
            place = group * pairs + pair
            query = q_ref[:, place * LANES:(place + 1) * LANES]
            scores = lax.dot_general(query, keys, (((1,), (1,)), ((), ())), preferred_element_type=jnp.float32)
            pieces = []
            for side in range(2):
                sink = sink_ref[2 * place + side]
                near = scores[:, 2 * side * rows:(2 * side + 1) * rows] * inv
                far = scores[:, (2 * side + 1) * rows:(2 * side + 2) * rows] * inv + bias
                score = jnp.where(own_mask, near, far)
                top = jnp.maximum(jnp.max(score, axis=1, keepdims=True), sink)
                expo = jnp.exp(score - top)
                denom = jnp.sum(expo, axis=1, keepdims=True) + jnp.exp(sink - top)
                weight = expo / denom
                pieces.append(jnp.where(own_mask, weight, 0.0).astype(jnp.bfloat16))
                pieces.append(jnp.where(own_mask, 0.0, weight).astype(jnp.bfloat16))
            out = jnp.dot(jnp.concatenate(pieces, axis=1), values, preferred_element_type=jnp.float32)
            ctx[:, place * LANES:(place + 1) * LANES] = out.astype(jnp.bfloat16)

    mine = jnp.dot(ctx[...], proj_ref[...], preferred_element_type=jnp.float32)
    weights[0].wait_recv()
    other = jnp.dot(ctx[...], proj_other[...], preferred_element_type=jnp.float32)
    part[...] = jnp.concatenate(
        [jnp.where(s == 0, mine, other), jnp.where(s == 0, other, mine)], axis=1
    )
    xsend[...] = part[pl.ds((1 - t) * half_rows, half_rows), :].astype(jnp.bfloat16)
    swap = remote(xsend, xrecv, xsem.at[0], xsem.at[1], across)
    swap.start()
    kept = part[pl.ds(t * half_rows, half_rows), :] + res_ref[pl.ds(t * half_rows, half_rows), :].astype(jnp.float32)
    experts = chips * 2
    ids = ids_ref[pl.ds(t * half_rows, half_rows), :]
    gw = gw_ref[pl.ds(t * half_rows, half_rows), :]
    base = width % LANES
    lane_half = lax.broadcasted_iota(jnp.int32, (half_rows, LANES), 1)
    gates = jnp.zeros((half_rows, LANES), jnp.float32)
    for k in range(ids.shape[1]):
        hit_high = lane_half == ids[:, k:k + 1] + base
        hit_low = lane_half == ids[:, k:k + 1] + (base + experts)
        value = gw[:, k:k + 1]
        high = value.astype(jnp.bfloat16).astype(jnp.float32)
        gates = gates + jnp.where(hit_high, high, 0.0) + jnp.where(hit_low, value - high, 0.0)
    swap.wait_recv()
    stream = kept + xrecv[...].astype(jnp.float32)
    stream_ref[...] = stream
    scale = lax.rsqrt(jnp.mean(stream * stream, axis=1, keepdims=True) + norm_eps)
    normed = (stream * scale * gain_ref[...]).astype(jnp.bfloat16)
    own = nbuf.at[e, s, t]
    own[:, :width] = normed
    edge = width // LANES * LANES
    tile = own[:, edge:edge + LANES].astype(jnp.float32)
    own[:, edge:edge + LANES] = jnp.where(lane_half < base, tile, gates).astype(jnp.bfloat16)

    def piece(ee, ss, tt, way, device):
        place = (ee * 2 + ss) * 2 + tt
        return remote(nbuf.at[ee, ss, tt], nbuf.at[ee, ss, tt], gsend.at[way, place], grecv.at[place], device)

    UP, DOWN, ACROSS, CORE = 0, 1, 2, 3
    when(has_up, lambda: piece(e, s, t, UP, up).start())
    when(has_down, lambda: piece(e, s, t, DOWN, down).start())
    piece(e, s, t, ACROSS, across).start()
    piece(e, s, t, CORE, core).start()

    def from_across(ee):
        got = piece(ee, s, 1 - t, CORE, core)
        got.wait_recv()
        got.start()

    for d in range(1, chips):
        def from_below(d=d):
            piece(e - d, s, t, UP, up).wait_recv()
            when(has_up, lambda: piece(e - d, s, t, UP, up).start())
            piece(e - d, s, t, ACROSS, across).start()
            piece(e - d, s, t, CORE, core).start()
        def from_above(d=d):
            piece(e + d, s, t, DOWN, down).wait_recv()
            when(has_down, lambda: piece(e + d, s, t, DOWN, down).start())
            piece(e + d, s, t, ACROSS, across).start()
            piece(e + d, s, t, CORE, core).start()
        when(e - d >= 0, from_below)
        when(e + d < chips, from_above)
        if d == 1:
            from_across(e)
        else:
            when(e - d + 1 >= 0, lambda d=d: from_across(e - d + 1))
            when(e + d - 1 < chips, lambda d=d: from_across(e + d - 1))
    d = chips - 1
    when(e - d >= 0, lambda: from_across(e - d))
    when(e + d < chips, lambda: from_across(e + d))
    for ee in range(chips):
        for tt in range(2):
            piece(ee, 1 - s, tt, CORE, core).wait_recv()
    for copy in weights[1:]:
        copy.wait_recv()
    for ee in range(chips):
        piece(ee, s, t, ACROSS, across).wait_send()
        piece(ee, s, t, CORE, core).wait_send()
        piece(ee, s, 1 - t, CORE, core).wait_send()
        when(has_up & (e >= ee), lambda ee=ee: piece(ee, s, t, UP, up).wait_send())
        when(has_down & (e <= ee), lambda ee=ee: piece(ee, s, t, DOWN, down).wait_send())
    for copy in weights:
        copy.wait_send()
    swap.wait_send()
    when(s == 0, lambda: kv_near.wait_send())
    when((s == 1) & has_up, lambda: kv_far.wait_send())


def back_kernel(
    chips, hidden_ref, down_ref, gate_ref, sh_ref, sdn_ref, stream_ref, out_ref,
    keep, dsend, drecv, xkeep, xsend, xrecv, zsend, zrecv,
    dsem_s, dsem_r, xsem_s, xsem_r, zsem_s, zsem_r,
):
    e, s, t = lax.axis_index("expert"), lax.axis_index("seq"), lax.axis_index("tensor")
    rows, col = out_ref.shape
    half_rows = rows // 2
    width = 2 * col
    base = width % LANES
    experts = 2 * chips
    core, across = {"seq": 1 - s}, {"tensor": 1 - t}
    up, down = {"expert": e + 1}, {"expert": e - 1}
    has_up, has_down = e < chips - 1, e > 0
    greet([(None, core), (None, across), (has_up, up), (has_down, down)])
    expert = e * 2 + s
    lane = lax.broadcasted_iota(jnp.int32, (rows, LANES), 1)
    wanted = (lane == base + expert) | (lane == base + experts + expert)
    order = [sorted(range(chips), key=lambda dest, me=me: -abs(dest - me)) for me in range(chips)]
    dests = [at_table([order[me][k] for me in range(chips)], e) for k in range(chips)]

    def block(dest, core_index):
        start = pl.multiple_of((dest * 2 + core_index) * rows, rows)
        gate = jnp.sum(
            jnp.where(wanted, gate_ref[pl.ds(start, rows), :].astype(jnp.float32), 0.0), axis=1, keepdims=True
        )
        return gate * jnp.dot(
            hidden_ref[pl.ds(start, rows), :], down_ref[...], preferred_element_type=jnp.float32
        )

    def to_core(k):
        return remote(dsend.at[k], drecv.at[k], dsem_s.at[k], dsem_r.at[k], core)

    def to_across(k):
        return remote(xsend.at[k], xrecv.at[k], xsem_s.at[k], xsem_r.at[k], across)

    def to_up(k):
        dest = dests[k]
        return remote(zsend.at[k], zrecv.at[0, dest], zsem_s.at[k], zsem_r.at[0, dest], up)

    def to_down(k):
        dest = dests[k]
        return remote(zsend.at[k], zrecv.at[1, dest], zsem_s.at[k], zsem_r.at[1, dest], down)

    def stage_a(k):
        dsend[k] = block(dests[k], 1 - s).astype(jnp.bfloat16)
        to_core(k).start()
        value = block(dests[k], s)
        keep[k] = value
        if k == chips - 1:
            shared = jnp.concatenate([
                jnp.dot(sh_ref[...], sdn_ref[h], preferred_element_type=jnp.float32) for h in range(2)
            ], axis=1)
            keep[k] += shared
            keep[k, pl.ds(t * half_rows, half_rows), :] += stream_ref[...]

    def stage_b(k):
        to_core(k).wait_recv()
        total = keep[k] + drecv[k].astype(jnp.float32)
        left, right = total[:, :col], total[:, col:]
        xsend[k] = jnp.where(t == 0, right, left).astype(jnp.bfloat16)
        to_across(k).start()
        xkeep[k] = jnp.where(t == 0, left, right)

    def stage_c(k):
        dest = dests[k]
        to_across(k).wait_recv()
        xkeep[k] += xrecv[k].astype(jnp.float32)

        def take(side, device_of):
            device_of(k).wait_recv()
            xkeep[k] += zrecv[side, dest].astype(jnp.float32)
        if k < chips - 1:
            when((dest > e) & has_down, lambda: take(0, to_up))
            when((dest < e) & has_up, lambda: take(1, to_down))
            zsend[k] = xkeep[k].astype(jnp.bfloat16)
            when(dest > e, lambda: to_up(k).start())
            when(dest < e, lambda: to_down(k).start())
        else:
            when(has_down, lambda: take(0, to_up))
            when(has_up, lambda: take(1, to_down))
            out_ref[...] = xkeep[k].astype(jnp.bfloat16)

    for step in range(chips + 2):
        if step < chips:
            stage_a(step)
        if 0 <= step - 1 < chips:
            stage_b(step - 1)
        if 0 <= step - 2 < chips:
            stage_c(step - 2)
    for k in range(chips):
        to_core(k).wait_send()
        to_across(k).wait_send()
        if k < chips - 1:
            to_up(k).wait_send()


def gathered(
    queries, keys_values, residual, sink_logits, norm_gain, out_proj, shared_gate_up, shared_down,
    expert_gate_up, expert_down, expert_ids, gate_weights,
):
    chips = lax.axis_size("expert")
    rows, width = residual.shape
    col = out_proj.shape[1]
    inner = out_proj.shape[0]
    depth = shared_gate_up.shape[0]
    sff = shared_gate_up.shape[2]
    wide = pad_lanes(width)
    kv_flat = keys_values.reshape(rows, -1)
    sgu = shared_gate_up.reshape(depth, 2 * sff)
    vmem = pl.BlockSpec(memory_space=pltpu.VMEM)
    smem = pl.BlockSpec(memory_space=pltpu.SMEM)
    bf16, f32 = jnp.bfloat16, jnp.float32
    dma = pltpu.SemaphoreType.DMA
    pieces = 4 * chips
    nbuf, stream, sgu_full, sdn_full = pl.pallas_call(
        functools.partial(front_kernel, chips),
        name="front",
        out_shape=(
            jax.ShapeDtypeStruct((chips, 2, 2, rows // 2, wide), bf16),
            jax.ShapeDtypeStruct((rows // 2, width), f32),
            jax.ShapeDtypeStruct((2 * depth, 2 * sff), bf16),
            jax.ShapeDtypeStruct((2, sff, col), bf16),
        ),
        in_specs=[vmem, vmem, vmem, smem] + [vmem] * 6,
        out_specs=(vmem,) * 4,
        scratch_shapes=[
            pltpu.VMEM(kv_flat.shape, bf16),
            pltpu.VMEM((inner, col), bf16),
            pltpu.VMEM((rows, inner), bf16),
            pltpu.VMEM((rows, width), f32),
            pltpu.VMEM((rows // 2, width), bf16),
            pltpu.VMEM((rows // 2, width), bf16),
            dma((3,)), dma((3,)), dma((2,)), dma((2,)), dma((4, pieces)), dma((pieces,)),
        ],
        compiler_params=pltpu.CompilerParams(
            collective_id=0, has_side_effects=True, vmem_limit_bytes=40 * 1024 * 1024
        ),
    )(queries, kv_flat, residual, sink_logits, norm_gain.reshape(1, -1), out_proj, sgu, shared_down,
      expert_ids, gate_weights)
    flat = nbuf.reshape(2 * chips * rows, wide)
    tokens = flat[:, :width]
    pre = jnp.einsum("pd,dhf->phf", tokens, expert_gate_up[0], preferred_element_type=f32)
    hidden = glu_act(pre[:, 0], pre[:, 1]).astype(bf16)
    block_index = lax.axis_index(("expert", "seq"))
    here = lax.dynamic_slice_in_dim(flat, block_index * rows, rows, 0)[:, :width]
    shared_pre = jnp.dot(here, sgu_full, preferred_element_type=f32)
    shared_hidden = glu_act(shared_pre[:, :sff], shared_pre[:, sff:]).astype(bf16)
    edge = width // LANES * LANES
    return pl.pallas_call(
        functools.partial(back_kernel, chips),
        name="back",
        out_shape=jax.ShapeDtypeStruct((rows, col), bf16),
        in_specs=[vmem] * 6,
        out_specs=vmem,
        scratch_shapes=[
            pltpu.VMEM((chips, rows, width), f32),
            pltpu.VMEM((chips, rows, width), bf16),
            pltpu.VMEM((chips, rows, width), bf16),
            pltpu.VMEM((chips, rows, col), f32),
            pltpu.VMEM((chips, rows, col), bf16),
            pltpu.VMEM((chips, rows, col), bf16),
            pltpu.VMEM((chips, rows, col), bf16),
            pltpu.VMEM((2, chips, rows, col), bf16),
            dma((chips,)), dma((chips,)), dma((chips,)), dma((chips,)), dma((chips,)), dma((2, chips)),
        ],
        compiler_params=pltpu.CompilerParams(
            collective_id=1, has_side_effects=True, vmem_limit_bytes=40 * 1024 * 1024
        ),
    )(hidden, expert_down[0], flat[:, edge:edge + LANES], shared_hidden, sdn_full, stream)


def fits(mesh, rows, width, top):
    devices = mesh.shape["expert"] * mesh.shape["seq"]
    capacity = max(2, 3 * rows * top // (2 * devices))
    spare = pad_lanes(width) - width
    return (
        rows <= 2 * capacity and rows == WINDOW and mesh.shape["tensor"] == 2 and mesh.shape["seq"] == 2
        and spare >= 2 * devices
    )


def solution(mesh):
    def body(*args):
        residual, expert_ids, gate_up = args[2], args[10], args[8]
        if gate_up.shape[0] == 1 and fits(mesh, residual.shape[0], residual.shape[1], expert_ids.shape[1]):
            return gathered(*args)
        return local(*args)

    in_specs = (
        P(("group", "expert", "seq"), "tensor"),
        P(("group", "expert", "seq"), "tensor", None),
        P(("group", "expert", "seq"), None),
        P("tensor"),
        P(),
        P("tensor", "seq"),
        P("seq", None, "tensor"),
        P("tensor", "seq"),
        P(("expert", "seq"), None, None, "tensor"),
        P(("expert", "seq"), "tensor", None),
        P(("group", "expert", "seq"), None),
        P(("group", "expert", "seq"), None),
    )
    out_specs = P(("group", "expert", "seq"), "tensor")
    return jax.shard_map(body, mesh=mesh, in_specs=in_specs, out_specs=out_specs, check_vma=False)
```

```python
import functools
import math

import jax
import jax.numpy as jnp
from jax import lax
from jax.experimental import pallas as pl
from jax.experimental.pallas import tpu as pltpu
from jax.sharding import PartitionSpec as P

WINDOW = 128


norm_eps = 1e-05
glu_alpha = 1.702


def shifted(value, axis, steps):
    count = lax.axis_size(axis)
    initial, last = (max(0, -steps), min(count, count - steps))
    return lax.ppermute(value, axis, [(source, source + steps) for source in range(initial, last)])


def glu_act(gate_pre, up_pre):
    return (up_pre + 1.0) * gate_pre * jax.nn.sigmoid(glu_alpha * gate_pre)


def attend_local(queries, keys_values, sink_logits, block_index):
    count_rows = queries.shape[0]
    kv_count = keys_values.shape[1]
    head_size = keys_values.shape[2] // 2
    group_size = queries.shape[1] // (head_size * kv_count)
    earlier = shifted(keys_values, ("expert", "seq"), 1)
    pair_block = jnp.concatenate([earlier, keys_values], axis=0)
    grouped = queries.reshape(count_rows, kv_count, group_size, head_size)
    key_part = pair_block[:, :, :head_size]
    value_part = pair_block[:, :, head_size:]
    scores = jnp.einsum(
        "pkgd,jkd->kgpj", grouped, key_part, preferred_element_type=jnp.float32
    ) / math.sqrt(head_size)
    query_pos = jnp.arange(count_rows, dtype=jnp.int32)[:, None]
    key_rel = jnp.arange(2 * count_rows, dtype=jnp.int32)[None, :] - count_rows
    distance = query_pos - key_rel
    visible = (distance >= 0) & (distance < WINDOW) & (block_index * count_rows + key_rel >= 0)
    scores = jnp.where(visible[None, None], scores, -jnp.inf)
    sink_term = sink_logits.reshape(kv_count, group_size)[:, :, None, None]
    top_score = jnp.maximum(jnp.max(scores, axis=-1, keepdims=True), sink_term)
    expo = jnp.exp(scores - top_score)
    denom = jnp.sum(expo, axis=-1, keepdims=True) + jnp.exp(sink_term - top_score)
    attn_weights = (expo / denom).astype(jnp.bfloat16)
    context = jnp.einsum(
        "kgpj,jkd->pkgd", attn_weights, value_part, preferred_element_type=jnp.float32
    )
    return context.astype(jnp.bfloat16).reshape(count_rows, kv_count * group_size * head_size)


def local(
    queries,
    keys_values,
    residual,
    sink_logits,
    norm_gain,
    out_proj,
    shared_gate_up,
    shared_down,
    expert_gate_up,
    expert_down,
    expert_ids,
    gate_weights,
):
    block_index = lax.axis_index(("expert", "seq"))
    context = attend_local(queries, keys_values, sink_logits, block_index)
    proj_full, shared_gu_full, shared_dn_full = (
        lax.all_gather(out_proj, "seq", axis=1, tiled=True),
        lax.all_gather(shared_gate_up, "seq", axis=0, tiled=True),
        lax.all_gather(shared_down, "seq", axis=1, tiled=True),
    )
    attn_part = jnp.dot(context, proj_full, preferred_element_type=jnp.float32)
    attn = lax.psum(attn_part.astype(jnp.bfloat16), "tensor").astype(jnp.float32)
    stream = residual.astype(jnp.float32) + attn
    scale = lax.rsqrt(jnp.mean(stream * stream, axis=-1, keepdims=True) + norm_eps)
    normed = (stream * scale * norm_gain).astype(jnp.bfloat16)
    shared_pre = jnp.einsum(
        "pd,dcf->pcf", normed, shared_gu_full, preferred_element_type=jnp.float32
    )
    shared_hidden = glu_act(shared_pre[:, 0], shared_pre[:, 1]).astype(jnp.bfloat16)
    shared_part = jnp.dot(shared_hidden, shared_dn_full, preferred_element_type=jnp.float32)
    count_rows = normed.shape[0]
    width = normed.shape[1]
    top_count = expert_ids.shape[1]
    expert_count = expert_gate_up.shape[0] * lax.axis_size(("expert", "seq"))
    capacity = max(2, 3 * count_rows * top_count // (2 * expert_count))
    tensor_size = lax.axis_size("tensor")
    col_width = width // tensor_size
    col_start = lax.axis_index("tensor") * col_width
    flat_ids = expert_ids.reshape(-1)
    assign_count = count_rows * top_count
    onehot = (flat_ids[:, None] == jnp.arange(expert_count, dtype=jnp.int32)[None, :]).astype(
        jnp.int32
    )
    ranks = jnp.sum((jnp.cumsum(onehot, axis=0) - 1) * onehot, axis=1)
    slots = flat_ids * capacity + ranks
    slot_source = (
        jnp.full((expert_count * capacity,), assign_count, jnp.int32)
        .at[slots]
        .set(jnp.arange(assign_count, dtype=jnp.int32))
    )
    token_of_slot = jnp.where(slot_source < assign_count, slot_source // top_count, count_rows)
    normed_padded = jnp.concatenate([normed, jnp.zeros((1, width), jnp.bfloat16)], axis=0)
    outgoing = normed_padded[token_of_slot].reshape(expert_count, capacity, width)
    arrived = lax.all_to_all(outgoing, ("expert", "seq"), split_axis=0, concat_axis=0, tiled=True)
    expert_pre = jnp.einsum(
        "scd,dhf->schf", arrived, expert_gate_up[0], preferred_element_type=jnp.float32
    )
    expert_hidden = glu_act(expert_pre[:, :, 0], expert_pre[:, :, 1]).astype(jnp.bfloat16)
    expert_part = jnp.einsum(
        "scf,fd->scd", expert_hidden, expert_down[0], preferred_element_type=jnp.float32
    )
    returned = lax.all_to_all(
        expert_part.astype(jnp.bfloat16), ("expert", "seq"), split_axis=0, concat_axis=0, tiled=True
    )
    picked = (
        returned.reshape(expert_count * capacity, width)[slots]
        .astype(jnp.float32)
        .reshape(count_rows, top_count, width)
    )
    routed = jnp.sum(picked * gate_weights[:, :, None], axis=1)
    shared_rounded = lax.optimization_barrier(shared_part.astype(jnp.bfloat16))
    combined = shared_rounded.astype(jnp.float32) + routed
    summed = lax.psum_scatter(
        combined.astype(jnp.bfloat16), "tensor", scatter_dimension=1, tiled=True
    ).astype(jnp.float32)
    stream_cols = lax.dynamic_slice_in_dim(stream, col_start, col_width, 1)
    return (stream_cols + summed).astype(jnp.bfloat16)


MESH_ID = pl.DeviceIdType.MESH
LANES = 128
CHUNKS = 2


def pad_lanes(count):
    return -(-count // LANES) * LANES


def at_table(table, index):
    value = jnp.int32(table[0])
    for place in range(1, len(table)):
        value = jnp.where(index == place, jnp.int32(table[place]), value)
    return value


def when(condition, action):
    pl.when(condition)(action)


def greet(others):
    barrier = pltpu.get_barrier_semaphore()
    for condition, device in others:
        def send(device=device):
            pl.semaphore_signal(barrier, inc=1, device_id=device, device_id_type=MESH_ID)
        send() if condition is None else when(condition, send)
    count = sum(jnp.int32(1) if condition is None else condition.astype(jnp.int32) for condition, _ in others)
    pl.semaphore_wait(barrier, count)


def remote(source, target, send_sem, recv_sem, device):
    return pltpu.make_async_remote_copy(
        src_ref=source, dst_ref=target, send_sem=send_sem, recv_sem=recv_sem,
        device_id=device, device_id_type=MESH_ID,
    )


def front_kernel(
    chips, q_ref, kv_ref, res_ref, sink_ref, gain_ref, proj_ref, sgu_ref, sdn_ref, ids_ref, gw_ref,
    nbuf, stream_ref, sgu_out, sdn_out,
    kv_prev, proj_other, ctx, part, xsend, xrecv, gscr,
    wsend, wrecv, kvsem, xsem, own_sem, gsend, grecv,
):
    e, s, t = lax.axis_index("expert"), lax.axis_index("seq"), lax.axis_index("tensor")
    rows = q_ref.shape[0]
    half_rows = rows // 2
    col = proj_ref.shape[0]
    depth = sgu_ref.shape[0]
    width = 2 * col
    core, across = {"seq": 1 - s}, {"tensor": 1 - t}
    up, down = {"expert": e + 1}, {"expert": e - 1}
    has_up, has_down = e < chips - 1, e > 0
    greet([
        (None, core), (None, across), (has_up, up), (has_down, down),
        ((s == 1) & has_up, {"expert": e + 1, "seq": 0}),
        ((s == 0) & has_down, {"expert": e - 1, "seq": 1}),
    ])
    first = (e == 0) & (s == 0)
    kv_near = remote(kv_ref, kv_prev, kvsem.at[0], kvsem.at[1], core)
    kv_far = remote(kv_ref, kv_prev, kvsem.at[0], kvsem.at[1], {"expert": e + 1, "seq": 0})
    when(s == 0, lambda: kv_near.start())
    when((s == 1) & has_up, lambda: kv_far.start())
    weights = [
        remote(proj_ref, proj_other, wsend.at[0], wrecv.at[0], core),
        remote(sgu_ref, sgu_out.at[pl.ds(s * depth, depth)], wsend.at[1], wrecv.at[1], core),
        remote(sdn_ref, sdn_out.at[s], wsend.at[2], wrecv.at[2], core),
    ]
    for copy in weights:
        copy.start()
    own_sgu = pltpu.make_async_copy(sgu_ref, sgu_out.at[pl.ds(s * depth, depth)], own_sem)
    own_sgu.start()
    sdn_out[s] = sdn_ref[...]

    def blank():
        kv_prev[...] = jnp.zeros_like(kv_prev)
    when(first, blank)
    when(jnp.logical_not(first), lambda: kv_near.wait_recv())

    lane = lax.broadcasted_iota(jnp.int32, (rows, LANES), 1)
    head = LANES // 2
    low = lane < head
    own_mask = lax.broadcasted_iota(jnp.int32, (rows, rows), 1) <= lax.broadcasted_iota(jnp.int32, (rows, rows), 0)
    bias = jnp.where(first, -1e30, 0.0).astype(jnp.float32)
    kv_count = kv_ref.shape[0] // rows
    to_row = lax.broadcasted_iota(jnp.int32, (kv_count * rows, kv_count * rows), 0)
    from_row = lax.broadcasted_iota(jnp.int32, (kv_count * rows, kv_count * rows), 1)
    sort_groups = (from_row == (to_row % rows) * kv_count + to_row // rows).astype(jnp.bfloat16)
    pairs = q_ref.shape[1] // LANES // kv_count
    inv = 1.0 / math.sqrt(head)

    def halves(whole, group):
        value = whole[group * rows:(group + 1) * rows]
        turned = pltpu.roll(value, head, 1)
        zero = jnp.zeros_like(value)
        return [
            jnp.where(low, value, zero).astype(jnp.bfloat16), jnp.where(low, zero, turned).astype(jnp.bfloat16),
            jnp.where(low, turned, zero).astype(jnp.bfloat16), jnp.where(low, zero, value).astype(jnp.bfloat16),
        ]

    kv_mine = jnp.dot(sort_groups, kv_ref[...], preferred_element_type=jnp.float32)
    kv_before = jnp.dot(sort_groups, kv_prev[...], preferred_element_type=jnp.float32)
    for group in range(kv_count):
        mine, before = halves(kv_mine, group), halves(kv_before, group)
        keys = jnp.concatenate([mine[0], before[0], mine[1], before[1]], axis=0)
        values = jnp.concatenate([mine[2], before[2], mine[3], before[3]], axis=0)
        for pair in range(pairs):
            place = group * pairs + pair
            query = q_ref[:, place * LANES:(place + 1) * LANES]
            scores = lax.dot_general(query, keys, (((1,), (1,)), ((), ())), preferred_element_type=jnp.float32)
            pieces = []
            for side in range(2):
                sink = sink_ref[2 * place + side]
                near = scores[:, 2 * side * rows:(2 * side + 1) * rows] * inv
                far = scores[:, (2 * side + 1) * rows:(2 * side + 2) * rows] * inv + bias
                score = jnp.where(own_mask, near, far)
                top = jnp.maximum(jnp.max(score, axis=1, keepdims=True), sink)
                expo = jnp.exp(score - top)
                denom = jnp.sum(expo, axis=1, keepdims=True) + jnp.exp(sink - top)
                weight = expo / denom
                pieces.append(jnp.where(own_mask, weight, 0.0).astype(jnp.bfloat16))
                pieces.append(jnp.where(own_mask, 0.0, weight).astype(jnp.bfloat16))
            out = jnp.dot(jnp.concatenate(pieces, axis=1), values, preferred_element_type=jnp.float32)
            ctx[:, place * LANES:(place + 1) * LANES] = out.astype(jnp.bfloat16)

    along = (((1,), (1,)), ((), ()))
    mine = lax.dot_general(ctx[...], proj_ref[...], along, preferred_element_type=jnp.float32)
    weights[0].wait_recv()
    other = lax.dot_general(ctx[...], proj_other[...], along, preferred_element_type=jnp.float32)
    part[...] = jnp.concatenate(
        [jnp.where(s == 0, mine, other), jnp.where(s == 0, other, mine)], axis=1
    )
    xsend[...] = part[pl.ds((1 - t) * half_rows, half_rows), :].astype(jnp.bfloat16)
    swap = remote(xsend, xrecv, xsem.at[0], xsem.at[1], across)
    swap.start()
    picked_row = lax.broadcasted_iota(jnp.int32, (half_rows, rows), 0) + t * half_rows
    pick = (lax.broadcasted_iota(jnp.int32, (half_rows, rows), 1) == picked_row).astype(jnp.bfloat16)
    kept = part[pl.ds(t * half_rows, half_rows), :] + lax.dot_general(
        pick, res_ref[...], along, preferred_element_type=jnp.float32
    )
    experts = chips * 2
    base = width % LANES
    lane_half = lax.broadcasted_iota(jnp.int32, (half_rows, LANES), 1)
    line = lax.broadcasted_iota(jnp.int32, (LANES, rows), 0)
    gates = jnp.zeros((LANES, rows), jnp.float32)
    for k in range(ids_ref.shape[0]):
        ids = ids_ref[k:k + 1, :] + base
        value = gw_ref[k:k + 1, :]
        high = value.astype(jnp.bfloat16).astype(jnp.float32)
        gates = gates + jnp.where(line == ids, high, 0.0) + jnp.where(line == ids + experts, value - high, 0.0)
    gscr[...] = gates.T
    swap.wait_recv()
    stream = kept + xrecv[...].astype(jnp.float32)
    stream_ref[...] = stream
    scale = lax.rsqrt(jnp.mean(stream * stream, axis=1, keepdims=True) + norm_eps)
    normed = (stream * scale * gain_ref[...].reshape(1, width)).astype(jnp.bfloat16)
    edge = width // LANES * LANES
    size = half_rows // CHUNKS

    def piece(ee, ss, tt, c, way, device):
        place = ((ee * 2 + ss) * 2 + tt) * CHUNKS + c
        part_of = nbuf.at[ee, ss, tt, c]
        return remote(part_of, part_of, gsend.at[way, place], grecv.at[place], device)

    UP, DOWN, ACROSS, CORE = 0, 1, 2, 3
    edge_gates = gscr[pl.ds(t * half_rows, half_rows), :]
    edge_tile = jnp.concatenate([normed[:, edge:], jnp.zeros((half_rows, edge + LANES - width), jnp.bfloat16)], axis=1)
    edge_tile = jnp.where(lane_half < base, edge_tile.astype(jnp.float32), edge_gates).astype(jnp.bfloat16)
    for c in range(CHUNKS):
        nbuf[e, s, t, c, :, :edge] = normed[c * size:(c + 1) * size, :edge]
        nbuf[e, s, t, c, :, edge:edge + LANES] = edge_tile[c * size:(c + 1) * size]
        piece(e, s, t, c, ACROSS, across).start()
        when(has_up, lambda c=c: piece(e, s, t, c, UP, up).start())
        when(has_down, lambda c=c: piece(e, s, t, c, DOWN, down).start())
        piece(e, s, t, c, CORE, core).start()

    def own_column(d):
        for c in range(CHUNKS):
            def from_below(c=c):
                piece(e - d, s, t, c, UP, up).wait_recv()
                when(has_up, lambda: piece(e - d, s, t, c, UP, up).start())
                if d > 1:
                    piece(e - d, s, t, c, ACROSS, across).start()
                piece(e - d, s, t, c, CORE, core).start()

            def from_above(c=c):
                piece(e + d, s, t, c, DOWN, down).wait_recv()
                when(has_down, lambda: piece(e + d, s, t, c, DOWN, down).start())
                if d > 1:
                    piece(e + d, s, t, c, ACROSS, across).start()
                piece(e + d, s, t, c, CORE, core).start()
            when(e - d >= 0, from_below)
            when(e + d < chips, from_above)

    def take(ee, c):
        got = piece(ee, s, 1 - t, c, CORE, core)
        got.wait_recv()
        got.start()

    def other_column(d):
        for c in range(CHUNKS):
            when(e - d >= 0, lambda c=c: take(e - d, c))
            when(e + d < chips, lambda c=c: take(e + d, c))

    for d in range(1, chips):
        own_column(d)
        if d == 1:
            for c in range(CHUNKS):
                take(e, c)
                when(has_up, lambda c=c: piece(e, s, 1 - t, c, UP, up).start())
                when(has_down, lambda c=c: piece(e, s, 1 - t, c, DOWN, down).start())
        else:
            other_column(d - 1)
    other_column(chips - 1)
    for ee in range(chips):
        for tt in range(2):
            for c in range(CHUNKS):
                piece(ee, 1 - s, tt, c, CORE, core).wait_recv()
    own_sgu.wait()
    for copy in weights[1:]:
        copy.wait_recv()
    for c in range(CHUNKS):
        for ee in range(chips):
            near = (e == ee - 1) | (e == ee + 1)
            when(jnp.logical_not(near), lambda ee=ee, c=c: piece(ee, s, t, c, ACROSS, across).wait_send())
            piece(ee, s, t, c, CORE, core).wait_send()
            piece(ee, s, 1 - t, c, CORE, core).wait_send()
            when(has_up & (e >= ee), lambda ee=ee, c=c: piece(ee, s, t, c, UP, up).wait_send())
            when(has_down & (e <= ee), lambda ee=ee, c=c: piece(ee, s, t, c, DOWN, down).wait_send())
        when(has_up, lambda c=c: piece(e, s, 1 - t, c, UP, up).wait_send())
        when(has_down, lambda c=c: piece(e, s, 1 - t, c, DOWN, down).wait_send())
    for copy in weights:
        copy.wait_send()
    swap.wait_send()
    when(s == 0, lambda: kv_near.wait_send())
    when((s == 1) & has_up, lambda: kv_far.wait_send())


def back_kernel(
    chips, hidden_ref, down_ref, gate_ref, sh_ref, sdn_ref, stream_ref, out_ref,
    keep, dsend, drecv, xkeep, xsend, xrecv, zsend, zrecv, orecv, spare,
    dsem_s, dsem_r, xsem_s, xsem_r, zsem_s, zsem_r, osem_r,
):
    e, s, t = lax.axis_index("expert"), lax.axis_index("seq"), lax.axis_index("tensor")
    rows, col = out_ref.shape
    half_rows = rows // 2
    width = 2 * col
    base = width % LANES
    experts = 2 * chips
    core, across = {"seq": 1 - s}, {"tensor": 1 - t}
    up, down = {"expert": e + 1}, {"expert": e - 1}
    has_up, has_down = e < chips - 1, e > 0
    greet([(None, core), (None, across), (has_up, up), (has_down, down)])
    expert = e * 2 + s
    lane = lax.broadcasted_iota(jnp.int32, (rows, LANES), 1)
    wanted = (lane == base + expert) | (lane == base + experts + expert)
    far_first = [sorted(range(chips), key=lambda dest, me=me: -abs(dest - me)) for me in range(chips)]
    near_first = [
        sorted(range(chips), key=lambda dest, me=me: (dest == me, abs(dest - me) != 1, -abs(dest - me)))
        for me in range(chips)
    ]
    later = [at_table([far_first[me][k] for me in range(chips)], e) for k in range(chips)]
    sooner = [at_table([near_first[me][k] for me in range(chips)], e) for k in range(chips)]
    size = rows // CHUNKS
    parts = [pl.ds(c * size, size) for c in range(CHUNKS)]
    along = (((1,), (1,)), ((), ()))

    def block(dest, core_index):
        start = pl.multiple_of((dest * 2 + core_index) * rows, rows)
        gate = jnp.sum(
            jnp.where(wanted, gate_ref[pl.ds(start, rows), :].astype(jnp.float32), 0.0), axis=1, keepdims=True
        )
        return gate * jnp.dot(
            hidden_ref[pl.ds(start, rows), :], down_ref[...], preferred_element_type=jnp.float32
        )

    def near_dest(dest):
        return (dest == e + 1) | (dest == e - 1)

    def to_core(dest):
        return remote(dsend.at[dest], drecv.at[dest], dsem_s.at[dest], dsem_r.at[dest], core)

    def to_across(dest, c):
        return remote(
            xsend.at[dest, parts[c]], xrecv.at[dest, parts[c]], xsem_s.at[dest, c], xsem_r.at[dest, c], across
        )

    def along_z(dest, side, c):
        return remote(
            zsend.at[dest, parts[c]], zrecv.at[side, dest, parts[c]], zsem_s.at[dest, c], zsem_r.at[side, dest, c],
            down if side else up,
        )

    def other_z(dest, side, c):
        return remote(
            xsend.at[dest, parts[c]], orecv.at[side, parts[c]], xsem_s.at[dest, c], osem_r.at[side, c],
            down if side else up,
        )

    def stage_a(dest, last):
        dsend[dest] = block(dest, 1 - s).astype(jnp.bfloat16)
        to_core(dest).start()
        value = block(dest, s)
        keep[dest] = value
        if last:
            shared = jnp.concatenate([
                lax.dot_general(sh_ref[...], sdn_ref[h], along, preferred_element_type=jnp.float32) for h in range(2)
            ], axis=1)
            keep[dest] += shared
            keep[dest, pl.ds(t * half_rows, half_rows), :] += stream_ref[...]

    def stage_b(dest, last):
        to_core(dest).wait_recv()
        for c in range(CHUNKS):
            total = keep[dest, parts[c]] + drecv[dest, parts[c]].astype(jnp.float32)
            left, right = total[:, :col], total[:, col:]
            xkeep[dest, parts[c]] = jnp.where(t == 0, left, right)
            other = jnp.where(t == 0, right, left)
            if last:
                spare[parts[c]] = other

                def add(side, c=c):
                    other_z(dest, side, c).wait_recv()
                    spare[parts[c]] += orecv[side, parts[c]].astype(jnp.float32)
                when(has_down, lambda: add(0))
                when(has_up, lambda: add(1))
                xsend[dest, parts[c]] = spare[parts[c]].astype(jnp.bfloat16)
                to_across(dest, c).start()
            else:
                xsend[dest, parts[c]] = other.astype(jnp.bfloat16)
                when(dest == e + 1, lambda c=c: other_z(dest, 0, c).start())
                when(dest == e - 1, lambda c=c: other_z(dest, 1, c).start())
                when(jnp.logical_not(near_dest(dest)), lambda c=c: to_across(dest, c).start())

    def stage_c(dest, last):
        for c in range(CHUNKS):
            def swap(c=c):
                to_across(dest, c).wait_recv()
                xkeep[dest, parts[c]] += xrecv[dest, parts[c]].astype(jnp.float32)

            def take(side, c=c):
                along_z(dest, side, c).wait_recv()
                xkeep[dest, parts[c]] += zrecv[side, dest, parts[c]].astype(jnp.float32)
            if last:
                swap()
                when(has_down, lambda: take(0))
                when(has_up, lambda: take(1))
                out_ref[parts[c]] = xkeep[dest, parts[c]].astype(jnp.bfloat16)
            else:
                when(jnp.logical_not(near_dest(dest)), swap)
                when((dest > e) & has_down, lambda: take(0))
                when((dest < e) & has_up, lambda: take(1))
                zsend[dest, parts[c]] = xkeep[dest, parts[c]].astype(jnp.bfloat16)
                when(dest > e, lambda c=c: along_z(dest, 0, c).start())
                when(dest < e, lambda c=c: along_z(dest, 1, c).start())

    for step in range(chips + 1):
        if step < chips:
            stage_a(sooner[step], step == chips - 1)
        if step >= 1:
            stage_b(sooner[step - 1], step == chips)
    for k in range(chips):
        stage_c(later[k], k == chips - 1)
    for k in range(chips):
        dest = sooner[k]
        to_core(dest).wait_send()
        for c in range(CHUNKS):
            to_across(dest, c).wait_send()
            if k < chips - 1:
                along_z(dest, 0, c).wait_send()


def gathered(
    queries, keys_values, residual, sink_logits, norm_gain, out_proj, shared_gate_up, shared_down,
    expert_gate_up, expert_down, expert_ids, gate_weights,
):
    chips = lax.axis_size("expert")
    rows, width = residual.shape
    col = out_proj.shape[1]
    inner = out_proj.shape[0]
    depth = shared_gate_up.shape[0]
    sff = shared_gate_up.shape[2]
    wide = pad_lanes(width)
    kv_flat = keys_values.reshape(-1, keys_values.shape[2])
    vmem = pl.BlockSpec(memory_space=pltpu.VMEM)
    smem = pl.BlockSpec(memory_space=pltpu.SMEM)
    bf16, f32 = jnp.bfloat16, jnp.float32
    dma = pltpu.SemaphoreType.DMA
    pieces = 4 * chips * CHUNKS
    nbuf, stream, sgu_full, sdn_full = pl.pallas_call(
        functools.partial(front_kernel, chips),
        name="front",
        out_shape=(
            jax.ShapeDtypeStruct((chips, 2, 2, CHUNKS, rows // 2 // CHUNKS, wide), bf16),
            jax.ShapeDtypeStruct((rows // 2, width), f32),
            jax.ShapeDtypeStruct((2 * depth, 2, sff), bf16),
            jax.ShapeDtypeStruct((2, col, sff), bf16),
        ),
        in_specs=[vmem, vmem, vmem, smem, vmem, vmem, pl.BlockSpec(memory_space=pltpu.HBM)] + [vmem] * 3,
        out_specs=(vmem,) * 4,
        scratch_shapes=[
            pltpu.VMEM(kv_flat.shape, bf16),
            pltpu.VMEM((col, inner), bf16),
            pltpu.VMEM((rows, inner), bf16),
            pltpu.VMEM((rows, width), f32),
            pltpu.VMEM((rows // 2, width), bf16),
            pltpu.VMEM((rows // 2, width), bf16),
            pltpu.VMEM((rows, LANES), f32),
            dma((3,)), dma((3,)), dma((2,)), dma((2,)), dma, dma((4, pieces)), dma((pieces,)),
        ],
        compiler_params=pltpu.CompilerParams(
            collective_id=0, has_side_effects=True, vmem_limit_bytes=40 * 1024 * 1024
        ),
    )(queries, kv_flat, residual.T, sink_logits, norm_gain, out_proj.T, shared_gate_up, shared_down.T,
      expert_ids.T, gate_weights.T)
    flat = nbuf.reshape(2 * chips * rows, wide)
    tokens = flat[:, :width]
    pre = jnp.einsum("pd,dhf->phf", tokens, expert_gate_up[0], preferred_element_type=f32)
    hidden = glu_act(pre[:, 0], pre[:, 1]).astype(bf16)
    block_index = lax.axis_index(("expert", "seq"))
    here = lax.dynamic_slice_in_dim(flat, block_index * rows, rows, 0)[:, :width]
    shared_pre = jnp.einsum("pd,dcf->pcf", here, sgu_full, preferred_element_type=f32)
    shared_hidden = glu_act(shared_pre[:, 0], shared_pre[:, 1]).astype(bf16)
    edge = width // LANES * LANES
    return pl.pallas_call(
        functools.partial(back_kernel, chips),
        name="back",
        out_shape=jax.ShapeDtypeStruct((rows, col), bf16),
        in_specs=[vmem] * 6,
        out_specs=vmem,
        scratch_shapes=[
            pltpu.VMEM((chips, rows, width), f32),
            pltpu.VMEM((chips, rows, width), bf16),
            pltpu.VMEM((chips, rows, width), bf16),
            pltpu.VMEM((chips, rows, col), f32),
            pltpu.VMEM((chips, rows, col), bf16),
            pltpu.VMEM((chips, rows, col), bf16),
            pltpu.VMEM((chips, rows, col), bf16),
            pltpu.VMEM((2, chips, rows, col), bf16),
            pltpu.VMEM((2, rows, col), bf16),
            pltpu.VMEM((rows, col), f32),
            dma((chips,)), dma((chips,)), dma((chips, CHUNKS)), dma((chips, CHUNKS)), dma((chips, CHUNKS)),
            dma((2, chips, CHUNKS)), dma((2, CHUNKS)),
        ],
        compiler_params=pltpu.CompilerParams(
            collective_id=1, has_side_effects=True, vmem_limit_bytes=40 * 1024 * 1024
        ),
    )(hidden, expert_down[0], flat[:, edge:edge + LANES], shared_hidden, sdn_full, stream)


def fits(mesh, rows, width, top):
    devices = mesh.shape["expert"] * mesh.shape["seq"]
    capacity = max(2, 3 * rows * top // (2 * devices))
    spare = pad_lanes(width) - width
    return (
        rows <= 2 * capacity and rows == WINDOW and mesh.shape["tensor"] == 2 and mesh.shape["seq"] == 2
        and spare >= 2 * devices
    )


def solution(mesh):
    def body(*args):
        residual, expert_ids, gate_up = args[2], args[10], args[8]
        if gate_up.shape[0] == 1 and fits(mesh, residual.shape[0], residual.shape[1], expert_ids.shape[1]):
            return gathered(*args)
        return local(*args)

    in_specs = (
        P(("group", "expert", "seq"), "tensor"),
        P(("group", "expert", "seq"), "tensor", None),
        P(("group", "expert", "seq"), None),
        P("tensor"),
        P(),
        P("tensor", "seq"),
        P("seq", None, "tensor"),
        P("tensor", "seq"),
        P(("expert", "seq"), None, None, "tensor"),
        P(("expert", "seq"), "tensor", None),
        P(("group", "expert", "seq"), None),
        P(("group", "expert", "seq"), None),
    )
    out_specs = P(("group", "expert", "seq"), "tensor")
    return jax.shard_map(body, mesh=mesh, in_specs=in_specs, out_specs=out_specs, check_vma=False)
```

```python
import functools
import math

import jax
import jax.numpy as jnp
from jax import lax
from jax.experimental import pallas as pl
from jax.experimental.pallas import tpu as pltpu
from jax.sharding import PartitionSpec as P

WINDOW = 128


norm_eps = 1e-05
glu_alpha = 1.702


def shifted(value, axis, steps):
    count = lax.axis_size(axis)
    initial, last = (max(0, -steps), min(count, count - steps))
    return lax.ppermute(value, axis, [(source, source + steps) for source in range(initial, last)])


def glu_act(gate_pre, up_pre):
    return (up_pre + 1.0) * gate_pre * jax.nn.sigmoid(glu_alpha * gate_pre)


def attend_local(queries, keys_values, sink_logits, block_index):
    count_rows = queries.shape[0]
    kv_count = keys_values.shape[1]
    head_size = keys_values.shape[2] // 2
    group_size = queries.shape[1] // (head_size * kv_count)
    earlier = shifted(keys_values, ("expert", "seq"), 1)
    pair_block = jnp.concatenate([earlier, keys_values], axis=0)
    grouped = queries.reshape(count_rows, kv_count, group_size, head_size)
    key_part = pair_block[:, :, :head_size]
    value_part = pair_block[:, :, head_size:]
    scores = jnp.einsum(
        "pkgd,jkd->kgpj", grouped, key_part, preferred_element_type=jnp.float32
    ) / math.sqrt(head_size)
    query_pos = jnp.arange(count_rows, dtype=jnp.int32)[:, None]
    key_rel = jnp.arange(2 * count_rows, dtype=jnp.int32)[None, :] - count_rows
    distance = query_pos - key_rel
    visible = (distance >= 0) & (distance < WINDOW) & (block_index * count_rows + key_rel >= 0)
    scores = jnp.where(visible[None, None], scores, -jnp.inf)
    sink_term = sink_logits.reshape(kv_count, group_size)[:, :, None, None]
    top_score = jnp.maximum(jnp.max(scores, axis=-1, keepdims=True), sink_term)
    expo = jnp.exp(scores - top_score)
    denom = jnp.sum(expo, axis=-1, keepdims=True) + jnp.exp(sink_term - top_score)
    attn_weights = (expo / denom).astype(jnp.bfloat16)
    context = jnp.einsum(
        "kgpj,jkd->pkgd", attn_weights, value_part, preferred_element_type=jnp.float32
    )
    return context.astype(jnp.bfloat16).reshape(count_rows, kv_count * group_size * head_size)


def local(
    queries,
    keys_values,
    residual,
    sink_logits,
    norm_gain,
    out_proj,
    shared_gate_up,
    shared_down,
    expert_gate_up,
    expert_down,
    expert_ids,
    gate_weights,
):
    block_index = lax.axis_index(("expert", "seq"))
    context = attend_local(queries, keys_values, sink_logits, block_index)
    proj_full, shared_gu_full, shared_dn_full = (
        lax.all_gather(out_proj, "seq", axis=1, tiled=True),
        lax.all_gather(shared_gate_up, "seq", axis=0, tiled=True),
        lax.all_gather(shared_down, "seq", axis=1, tiled=True),
    )
    attn_part = jnp.dot(context, proj_full, preferred_element_type=jnp.float32)
    attn = lax.psum(attn_part.astype(jnp.bfloat16), "tensor").astype(jnp.float32)
    stream = residual.astype(jnp.float32) + attn
    scale = lax.rsqrt(jnp.mean(stream * stream, axis=-1, keepdims=True) + norm_eps)
    normed = (stream * scale * norm_gain).astype(jnp.bfloat16)
    shared_pre = jnp.einsum(
        "pd,dcf->pcf", normed, shared_gu_full, preferred_element_type=jnp.float32
    )
    shared_hidden = glu_act(shared_pre[:, 0], shared_pre[:, 1]).astype(jnp.bfloat16)
    shared_part = jnp.dot(shared_hidden, shared_dn_full, preferred_element_type=jnp.float32)
    count_rows = normed.shape[0]
    width = normed.shape[1]
    top_count = expert_ids.shape[1]
    expert_count = expert_gate_up.shape[0] * lax.axis_size(("expert", "seq"))
    capacity = max(2, 3 * count_rows * top_count // (2 * expert_count))
    tensor_size = lax.axis_size("tensor")
    col_width = width // tensor_size
    col_start = lax.axis_index("tensor") * col_width
    flat_ids = expert_ids.reshape(-1)
    assign_count = count_rows * top_count
    onehot = (flat_ids[:, None] == jnp.arange(expert_count, dtype=jnp.int32)[None, :]).astype(
        jnp.int32
    )
    ranks = jnp.sum((jnp.cumsum(onehot, axis=0) - 1) * onehot, axis=1)
    slots = flat_ids * capacity + ranks
    slot_source = (
        jnp.full((expert_count * capacity,), assign_count, jnp.int32)
        .at[slots]
        .set(jnp.arange(assign_count, dtype=jnp.int32))
    )
    token_of_slot = jnp.where(slot_source < assign_count, slot_source // top_count, count_rows)
    normed_padded = jnp.concatenate([normed, jnp.zeros((1, width), jnp.bfloat16)], axis=0)
    outgoing = normed_padded[token_of_slot].reshape(expert_count, capacity, width)
    arrived = lax.all_to_all(outgoing, ("expert", "seq"), split_axis=0, concat_axis=0, tiled=True)
    expert_pre = jnp.einsum(
        "scd,dhf->schf", arrived, expert_gate_up[0], preferred_element_type=jnp.float32
    )
    expert_hidden = glu_act(expert_pre[:, :, 0], expert_pre[:, :, 1]).astype(jnp.bfloat16)
    expert_part = jnp.einsum(
        "scf,fd->scd", expert_hidden, expert_down[0], preferred_element_type=jnp.float32
    )
    returned = lax.all_to_all(
        expert_part.astype(jnp.bfloat16), ("expert", "seq"), split_axis=0, concat_axis=0, tiled=True
    )
    picked = (
        returned.reshape(expert_count * capacity, width)[slots]
        .astype(jnp.float32)
        .reshape(count_rows, top_count, width)
    )
    routed = jnp.sum(picked * gate_weights[:, :, None], axis=1)
    shared_rounded = lax.optimization_barrier(shared_part.astype(jnp.bfloat16))
    combined = shared_rounded.astype(jnp.float32) + routed
    summed = lax.psum_scatter(
        combined.astype(jnp.bfloat16), "tensor", scatter_dimension=1, tiled=True
    ).astype(jnp.float32)
    stream_cols = lax.dynamic_slice_in_dim(stream, col_start, col_width, 1)
    return (stream_cols + summed).astype(jnp.bfloat16)


MESH_ID = pl.DeviceIdType.MESH
LANES = 128
CHUNKS = 4


def pad_lanes(count):
    return -(-count // LANES) * LANES


def at_table(table, index):
    value = jnp.int32(table[0])
    for place in range(1, len(table)):
        value = jnp.where(index == place, jnp.int32(table[place]), value)
    return value


def when(condition, action):
    pl.when(condition)(action)


def greet(others):
    barrier = pltpu.get_barrier_semaphore()
    for condition, device in others:
        def send(device=device):
            pl.semaphore_signal(barrier, inc=1, device_id=device, device_id_type=MESH_ID)
        send() if condition is None else when(condition, send)
    count = sum(jnp.int32(1) if condition is None else condition.astype(jnp.int32) for condition, _ in others)
    pl.semaphore_wait(barrier, count)


def remote(source, target, send_sem, recv_sem, device):
    return pltpu.make_async_remote_copy(
        src_ref=source, dst_ref=target, send_sem=send_sem, recv_sem=recv_sem,
        device_id=device, device_id_type=MESH_ID,
    )


def front_kernel(
    chips, q_ref, kv_ref, res_ref, sink_ref, gain_ref, proj_ref, sgu_ref, sdn_ref, ids_ref, gw_ref,
    nbuf, stream_ref, sgu_out, sdn_out,
    kv_prev, proj_other, ctx, part, xsend, xrecv, gscr,
    wsend, wrecv, kvsem, xsem, own_sem, gsend, grecv,
):
    e, s, t = lax.axis_index("expert"), lax.axis_index("seq"), lax.axis_index("tensor")
    rows = q_ref.shape[0]
    half_rows = rows // 2
    col = proj_ref.shape[0]
    depth = sgu_ref.shape[0]
    width = 2 * col
    core, across = {"seq": 1 - s}, {"tensor": 1 - t}
    up, down = {"expert": e + 1}, {"expert": e - 1}
    has_up, has_down = e < chips - 1, e > 0
    greet([
        (None, core), (None, across), (has_up, up), (has_down, down),
        ((s == 1) & has_up, {"expert": e + 1, "seq": 0}),
        ((s == 0) & has_down, {"expert": e - 1, "seq": 1}),
    ])
    first = (e == 0) & (s == 0)
    kv_near = remote(kv_ref, kv_prev, kvsem.at[0], kvsem.at[1], core)
    kv_far = remote(kv_ref, kv_prev, kvsem.at[0], kvsem.at[1], {"expert": e + 1, "seq": 0})
    when(s == 0, lambda: kv_near.start())
    when((s == 1) & has_up, lambda: kv_far.start())
    weights = [
        remote(proj_ref, proj_other, wsend.at[0], wrecv.at[0], core),
        remote(sgu_ref, sgu_out.at[pl.ds(s * depth, depth)], wsend.at[1], wrecv.at[1], core),
        remote(sdn_ref, sdn_out.at[s], wsend.at[2], wrecv.at[2], core),
    ]
    for copy in weights:
        copy.start()
    own_sgu = pltpu.make_async_copy(sgu_ref, sgu_out.at[pl.ds(s * depth, depth)], own_sem)
    own_sgu.start()
    sdn_out[s] = sdn_ref[...]

    def blank():
        kv_prev[...] = jnp.zeros_like(kv_prev)
    when(first, blank)
    when(jnp.logical_not(first), lambda: kv_near.wait_recv())

    lane = lax.broadcasted_iota(jnp.int32, (rows, LANES), 1)
    head = LANES // 2
    low = lane < head
    own_mask = lax.broadcasted_iota(jnp.int32, (rows, rows), 1) <= lax.broadcasted_iota(jnp.int32, (rows, rows), 0)
    bias = jnp.where(first, -1e30, 0.0).astype(jnp.float32)
    kv_count = kv_ref.shape[0] // rows
    to_row = lax.broadcasted_iota(jnp.int32, (kv_count * rows, kv_count * rows), 0)
    from_row = lax.broadcasted_iota(jnp.int32, (kv_count * rows, kv_count * rows), 1)
    sort_groups = (from_row == (to_row % rows) * kv_count + to_row // rows).astype(jnp.bfloat16)
    pairs = q_ref.shape[1] // LANES // kv_count
    inv = 1.0 / math.sqrt(head)

    def halves(whole, group):
        value = whole[group * rows:(group + 1) * rows]
        turned = pltpu.roll(value, head, 1)
        zero = jnp.zeros_like(value)
        return [
            jnp.where(low, value, zero).astype(jnp.bfloat16), jnp.where(low, zero, turned).astype(jnp.bfloat16),
            jnp.where(low, turned, zero).astype(jnp.bfloat16), jnp.where(low, zero, value).astype(jnp.bfloat16),
        ]

    kv_mine = jnp.dot(sort_groups, kv_ref[...], preferred_element_type=jnp.float32)
    kv_before = jnp.dot(sort_groups, kv_prev[...], preferred_element_type=jnp.float32)
    for group in range(kv_count):
        mine, before = halves(kv_mine, group), halves(kv_before, group)
        keys = jnp.concatenate([mine[0], before[0], mine[1], before[1]], axis=0)
        values = jnp.concatenate([mine[2], before[2], mine[3], before[3]], axis=0)
        for pair in range(pairs):
            place = group * pairs + pair
            query = q_ref[:, place * LANES:(place + 1) * LANES]
            scores = lax.dot_general(query, keys, (((1,), (1,)), ((), ())), preferred_element_type=jnp.float32)
            pieces = []
            for side in range(2):
                sink = sink_ref[2 * place + side]
                near = scores[:, 2 * side * rows:(2 * side + 1) * rows] * inv
                far = scores[:, (2 * side + 1) * rows:(2 * side + 2) * rows] * inv + bias
                score = jnp.where(own_mask, near, far)
                top = jnp.maximum(jnp.max(score, axis=1, keepdims=True), sink)
                expo = jnp.exp(score - top)
                denom = jnp.sum(expo, axis=1, keepdims=True) + jnp.exp(sink - top)
                weight = expo / denom
                pieces.append(jnp.where(own_mask, weight, 0.0).astype(jnp.bfloat16))
                pieces.append(jnp.where(own_mask, 0.0, weight).astype(jnp.bfloat16))
            out = jnp.dot(jnp.concatenate(pieces, axis=1), values, preferred_element_type=jnp.float32)
            ctx[:, place * LANES:(place + 1) * LANES] = out.astype(jnp.bfloat16)

    along = (((1,), (1,)), ((), ()))
    mine = lax.dot_general(ctx[...], proj_ref[...], along, preferred_element_type=jnp.float32)
    weights[0].wait_recv()
    other = lax.dot_general(ctx[...], proj_other[...], along, preferred_element_type=jnp.float32)
    part[...] = jnp.concatenate(
        [jnp.where(s == 0, mine, other), jnp.where(s == 0, other, mine)], axis=1
    )
    xsend[...] = part[pl.ds((1 - t) * half_rows, half_rows), :].astype(jnp.bfloat16)
    swap = remote(xsend, xrecv, xsem.at[0], xsem.at[1], across)
    swap.start()
    picked_row = lax.broadcasted_iota(jnp.int32, (half_rows, rows), 0) + t * half_rows
    pick = (lax.broadcasted_iota(jnp.int32, (half_rows, rows), 1) == picked_row).astype(jnp.bfloat16)
    kept = part[pl.ds(t * half_rows, half_rows), :] + lax.dot_general(
        pick, res_ref[...], along, preferred_element_type=jnp.float32
    )
    experts = chips * 2
    base = width % LANES
    lane_half = lax.broadcasted_iota(jnp.int32, (half_rows, LANES), 1)
    line = lax.broadcasted_iota(jnp.int32, (LANES, rows), 0)
    gates = jnp.zeros((LANES, rows), jnp.float32)
    for k in range(ids_ref.shape[0]):
        ids = ids_ref[k:k + 1, :] + base
        value = gw_ref[k:k + 1, :]
        high = value.astype(jnp.bfloat16).astype(jnp.float32)
        gates = gates + jnp.where(line == ids, high, 0.0) + jnp.where(line == ids + experts, value - high, 0.0)
    gscr[...] = gates.T
    swap.wait_recv()
    stream = kept + xrecv[...].astype(jnp.float32)
    stream_ref[...] = stream
    scale = lax.rsqrt(jnp.mean(stream * stream, axis=1, keepdims=True) + norm_eps)
    normed = (stream * scale * gain_ref[...].reshape(1, width)).astype(jnp.bfloat16)
    edge = width // LANES * LANES
    size = half_rows // CHUNKS

    def piece(ee, ss, tt, c, way, device):
        place = ((ee * 2 + ss) * 2 + tt) * CHUNKS + c
        part_of = nbuf.at[ee, ss, tt, c]
        return remote(part_of, part_of, gsend.at[way, place], grecv.at[place], device)

    UP, DOWN, ACROSS, CORE = 0, 1, 2, 3
    edge_gates = gscr[pl.ds(t * half_rows, half_rows), :]
    edge_tile = jnp.concatenate([normed[:, edge:], jnp.zeros((half_rows, edge + LANES - width), jnp.bfloat16)], axis=1)
    edge_tile = jnp.where(lane_half < base, edge_tile.astype(jnp.float32), edge_gates).astype(jnp.bfloat16)
    for c in range(CHUNKS):
        nbuf[e, s, t, c, :, :edge] = normed[c * size:(c + 1) * size, :edge]
        nbuf[e, s, t, c, :, edge:edge + LANES] = edge_tile[c * size:(c + 1) * size]
        piece(e, s, t, c, ACROSS, across).start()
        when(has_up, lambda c=c: piece(e, s, t, c, UP, up).start())
        when(has_down, lambda c=c: piece(e, s, t, c, DOWN, down).start())
        piece(e, s, t, c, CORE, core).start()

    def own_column(d):
        for c in range(CHUNKS):
            def from_below(c=c):
                piece(e - d, s, t, c, UP, up).wait_recv()
                when(has_up, lambda: piece(e - d, s, t, c, UP, up).start())
                if d > 1:
                    piece(e - d, s, t, c, ACROSS, across).start()
                piece(e - d, s, t, c, CORE, core).start()

            def from_above(c=c):
                piece(e + d, s, t, c, DOWN, down).wait_recv()
                when(has_down, lambda: piece(e + d, s, t, c, DOWN, down).start())
                if d > 1:
                    piece(e + d, s, t, c, ACROSS, across).start()
                piece(e + d, s, t, c, CORE, core).start()
            when(e - d >= 0, from_below)
            when(e + d < chips, from_above)

    def take(ee, c):
        got = piece(ee, s, 1 - t, c, CORE, core)
        got.wait_recv()
        got.start()

    def other_column(d):
        for c in range(CHUNKS):
            when(e - d >= 0, lambda c=c: take(e - d, c))
            when(e + d < chips, lambda c=c: take(e + d, c))

    for d in range(1, chips):
        own_column(d)
        if d == 1:
            for c in range(CHUNKS):
                take(e, c)
                when(has_up, lambda c=c: piece(e, s, 1 - t, c, UP, up).start())
                when(has_down, lambda c=c: piece(e, s, 1 - t, c, DOWN, down).start())
        else:
            other_column(d - 1)
    other_column(chips - 1)
    for ee in range(chips):
        for tt in range(2):
            for c in range(CHUNKS):
                piece(ee, 1 - s, tt, c, CORE, core).wait_recv()
    own_sgu.wait()
    for copy in weights[1:]:
        copy.wait_recv()
    for c in range(CHUNKS):
        for ee in range(chips):
            near = (e == ee - 1) | (e == ee + 1)
            when(jnp.logical_not(near), lambda ee=ee, c=c: piece(ee, s, t, c, ACROSS, across).wait_send())
            piece(ee, s, t, c, CORE, core).wait_send()
            piece(ee, s, 1 - t, c, CORE, core).wait_send()
            when(has_up & (e >= ee), lambda ee=ee, c=c: piece(ee, s, t, c, UP, up).wait_send())
            when(has_down & (e <= ee), lambda ee=ee, c=c: piece(ee, s, t, c, DOWN, down).wait_send())
        when(has_up, lambda c=c: piece(e, s, 1 - t, c, UP, up).wait_send())
        when(has_down, lambda c=c: piece(e, s, 1 - t, c, DOWN, down).wait_send())
    for copy in weights:
        copy.wait_send()
    swap.wait_send()
    when(s == 0, lambda: kv_near.wait_send())
    when((s == 1) & has_up, lambda: kv_far.wait_send())


def back_kernel(
    chips, hidden_ref, down_ref, gate_ref, sh_ref, sdn_ref, stream_ref, out_ref,
    keep, dsend, drecv, xkeep, xsend, xrecv, zsend, zrecv, orecv, spare,
    dsem_s, dsem_r, xsem_s, xsem_r, zsem_s, zsem_r, osem_r,
):
    e, s, t = lax.axis_index("expert"), lax.axis_index("seq"), lax.axis_index("tensor")
    rows, col = out_ref.shape
    half_rows = rows // 2
    width = 2 * col
    base = width % LANES
    experts = 2 * chips
    core, across = {"seq": 1 - s}, {"tensor": 1 - t}
    up, down = {"expert": e + 1}, {"expert": e - 1}
    has_up, has_down = e < chips - 1, e > 0
    greet([(None, core), (None, across), (has_up, up), (has_down, down)])
    expert = e * 2 + s
    lane = lax.broadcasted_iota(jnp.int32, (rows, LANES), 1)
    wanted = (lane == base + expert) | (lane == base + experts + expert)
    far_first = [sorted(range(chips), key=lambda dest, me=me: -abs(dest - me)) for me in range(chips)]
    near_first = [
        sorted(range(chips), key=lambda dest, me=me: (dest == me, abs(dest - me) != 1, -abs(dest - me)))
        for me in range(chips)
    ]
    later = [at_table([far_first[me][k] for me in range(chips)], e) for k in range(chips)]
    sooner = [at_table([near_first[me][k] for me in range(chips)], e) for k in range(chips)]
    size = rows // CHUNKS
    parts = [pl.ds(c * size, size) for c in range(CHUNKS)]
    along = (((1,), (1,)), ((), ()))

    def block(dest, core_index):
        start = pl.multiple_of((dest * 2 + core_index) * rows, rows)
        gate = jnp.sum(
            jnp.where(wanted, gate_ref[pl.ds(start, rows), :].astype(jnp.float32), 0.0), axis=1, keepdims=True
        )
        return gate * jnp.dot(
            hidden_ref[pl.ds(start, rows), :], down_ref[...], preferred_element_type=jnp.float32
        )

    def near_dest(dest):
        return (dest == e + 1) | (dest == e - 1)

    def to_core(dest):
        return remote(dsend.at[dest], drecv.at[dest], dsem_s.at[dest], dsem_r.at[dest], core)

    def to_across(dest, c):
        return remote(
            xsend.at[dest, parts[c]], xrecv.at[dest, parts[c]], xsem_s.at[dest, c], xsem_r.at[dest, c], across
        )

    def along_z(dest, side, c):
        return remote(
            zsend.at[dest, parts[c]], zrecv.at[side, dest, parts[c]], zsem_s.at[dest, c], zsem_r.at[side, dest, c],
            down if side else up,
        )

    def other_z(dest, side, c):
        return remote(
            xsend.at[dest, parts[c]], orecv.at[side, parts[c]], xsem_s.at[dest, c], osem_r.at[side, c],
            down if side else up,
        )

    def stage_a(dest, last):
        dsend[dest] = block(dest, 1 - s).astype(jnp.bfloat16)
        to_core(dest).start()
        value = block(dest, s)
        keep[dest] = value
        if last:
            shared = jnp.concatenate([
                lax.dot_general(sh_ref[...], sdn_ref[h], along, preferred_element_type=jnp.float32) for h in range(2)
            ], axis=1)
            keep[dest] += shared
            keep[dest, pl.ds(t * half_rows, half_rows), :] += stream_ref[...]

    def stage_b(dest, last):
        to_core(dest).wait_recv()
        for c in range(CHUNKS):
            total = keep[dest, parts[c]] + drecv[dest, parts[c]].astype(jnp.float32)
            left, right = total[:, :col], total[:, col:]
            xkeep[dest, parts[c]] = jnp.where(t == 0, left, right)
            other = jnp.where(t == 0, right, left)
            if last:
                spare[parts[c]] = other

                def add(side, c=c):
                    other_z(dest, side, c).wait_recv()
                    spare[parts[c]] += orecv[side, parts[c]].astype(jnp.float32)
                when(has_down, lambda: add(0))
                when(has_up, lambda: add(1))
                xsend[dest, parts[c]] = spare[parts[c]].astype(jnp.bfloat16)
                to_across(dest, c).start()
            else:
                xsend[dest, parts[c]] = other.astype(jnp.bfloat16)
                when(dest == e + 1, lambda c=c: other_z(dest, 0, c).start())
                when(dest == e - 1, lambda c=c: other_z(dest, 1, c).start())
                when(jnp.logical_not(near_dest(dest)), lambda c=c: to_across(dest, c).start())

    def stage_c(dest, last):
        for c in range(CHUNKS):
            def swap(c=c):
                to_across(dest, c).wait_recv()
                xkeep[dest, parts[c]] += xrecv[dest, parts[c]].astype(jnp.float32)

            def take(side, c=c):
                along_z(dest, side, c).wait_recv()
                xkeep[dest, parts[c]] += zrecv[side, dest, parts[c]].astype(jnp.float32)
            if last:
                swap()
                when(has_down, lambda: take(0))
                when(has_up, lambda: take(1))
                out_ref[parts[c]] = xkeep[dest, parts[c]].astype(jnp.bfloat16)
            else:
                when(jnp.logical_not(near_dest(dest)), swap)
                when((dest > e) & has_down, lambda: take(0))
                when((dest < e) & has_up, lambda: take(1))
                zsend[dest, parts[c]] = xkeep[dest, parts[c]].astype(jnp.bfloat16)
                when(dest > e, lambda c=c: along_z(dest, 0, c).start())
                when(dest < e, lambda c=c: along_z(dest, 1, c).start())

    for step in range(chips + 1):
        if step < chips:
            stage_a(sooner[step], step == chips - 1)
        if step >= 1:
            stage_b(sooner[step - 1], step == chips)
    for k in range(chips):
        stage_c(later[k], k == chips - 1)
    for k in range(chips):
        dest = sooner[k]
        to_core(dest).wait_send()
        for c in range(CHUNKS):
            to_across(dest, c).wait_send()
            if k < chips - 1:
                along_z(dest, 0, c).wait_send()


def gathered(
    queries, keys_values, residual, sink_logits, norm_gain, out_proj, shared_gate_up, shared_down,
    expert_gate_up, expert_down, expert_ids, gate_weights,
):
    chips = lax.axis_size("expert")
    rows, width = residual.shape
    col = out_proj.shape[1]
    inner = out_proj.shape[0]
    depth = shared_gate_up.shape[0]
    sff = shared_gate_up.shape[2]
    wide = pad_lanes(width)
    kv_flat = keys_values.reshape(-1, keys_values.shape[2])
    vmem = pl.BlockSpec(memory_space=pltpu.VMEM)
    smem = pl.BlockSpec(memory_space=pltpu.SMEM)
    bf16, f32 = jnp.bfloat16, jnp.float32
    dma = pltpu.SemaphoreType.DMA
    pieces = 4 * chips * CHUNKS
    nbuf, stream, sgu_full, sdn_full = pl.pallas_call(
        functools.partial(front_kernel, chips),
        name="front",
        out_shape=(
            jax.ShapeDtypeStruct((chips, 2, 2, CHUNKS, rows // 2 // CHUNKS, wide), bf16),
            jax.ShapeDtypeStruct((rows // 2, width), f32),
            jax.ShapeDtypeStruct((2 * depth, 2, sff), bf16),
            jax.ShapeDtypeStruct((2, col, sff), bf16),
        ),
        in_specs=[vmem, vmem, vmem, smem, vmem, vmem, pl.BlockSpec(memory_space=pltpu.HBM)] + [vmem] * 3,
        out_specs=(vmem,) * 4,
        scratch_shapes=[
            pltpu.VMEM(kv_flat.shape, bf16),
            pltpu.VMEM((col, inner), bf16),
            pltpu.VMEM((rows, inner), bf16),
            pltpu.VMEM((rows, width), f32),
            pltpu.VMEM((rows // 2, width), bf16),
            pltpu.VMEM((rows // 2, width), bf16),
            pltpu.VMEM((rows, LANES), f32),
            dma((3,)), dma((3,)), dma((2,)), dma((2,)), dma, dma((4, pieces)), dma((pieces,)),
        ],
        compiler_params=pltpu.CompilerParams(
            collective_id=0, has_side_effects=True, vmem_limit_bytes=40 * 1024 * 1024
        ),
    )(queries, kv_flat, residual.T, sink_logits, norm_gain, out_proj.T, shared_gate_up, shared_down.T,
      expert_ids.T, gate_weights.T)
    flat = nbuf.reshape(2 * chips * rows, wide)
    tokens = flat[:, :width]
    pre = jnp.einsum("pd,dhf->phf", tokens, expert_gate_up[0], preferred_element_type=f32)
    hidden = glu_act(pre[:, 0], pre[:, 1]).astype(bf16)
    block_index = lax.axis_index(("expert", "seq"))
    here = lax.dynamic_slice_in_dim(flat, block_index * rows, rows, 0)[:, :width]
    shared_pre = jnp.einsum("pd,dcf->pcf", here, sgu_full, preferred_element_type=f32)
    shared_hidden = glu_act(shared_pre[:, 0], shared_pre[:, 1]).astype(bf16)
    edge = width // LANES * LANES
    return pl.pallas_call(
        functools.partial(back_kernel, chips),
        name="back",
        out_shape=jax.ShapeDtypeStruct((rows, col), bf16),
        in_specs=[vmem] * 6,
        out_specs=vmem,
        scratch_shapes=[
            pltpu.VMEM((chips, rows, width), f32),
            pltpu.VMEM((chips, rows, width), bf16),
            pltpu.VMEM((chips, rows, width), bf16),
            pltpu.VMEM((chips, rows, col), f32),
            pltpu.VMEM((chips, rows, col), bf16),
            pltpu.VMEM((chips, rows, col), bf16),
            pltpu.VMEM((chips, rows, col), bf16),
            pltpu.VMEM((2, chips, rows, col), bf16),
            pltpu.VMEM((2, rows, col), bf16),
            pltpu.VMEM((rows, col), f32),
            dma((chips,)), dma((chips,)), dma((chips, CHUNKS)), dma((chips, CHUNKS)), dma((chips, CHUNKS)),
            dma((2, chips, CHUNKS)), dma((2, CHUNKS)),
        ],
        compiler_params=pltpu.CompilerParams(
            collective_id=1, has_side_effects=True, vmem_limit_bytes=40 * 1024 * 1024
        ),
    )(hidden, expert_down[0], flat[:, edge:edge + LANES], shared_hidden, sdn_full, stream)


def fits(mesh, rows, width, top):
    devices = mesh.shape["expert"] * mesh.shape["seq"]
    capacity = max(2, 3 * rows * top // (2 * devices))
    spare = pad_lanes(width) - width
    return (
        rows <= 2 * capacity and rows == WINDOW and mesh.shape["tensor"] == 2 and mesh.shape["seq"] == 2
        and spare >= 2 * devices
    )


def solution(mesh):
    def body(*args):
        residual, expert_ids, gate_up = args[2], args[10], args[8]
        if gate_up.shape[0] == 1 and fits(mesh, residual.shape[0], residual.shape[1], expert_ids.shape[1]):
            return gathered(*args)
        return local(*args)

    in_specs = (
        P(("group", "expert", "seq"), "tensor"),
        P(("group", "expert", "seq"), "tensor", None),
        P(("group", "expert", "seq"), None),
        P("tensor"),
        P(),
        P("tensor", "seq"),
        P("seq", None, "tensor"),
        P("tensor", "seq"),
        P(("expert", "seq"), None, None, "tensor"),
        P(("expert", "seq"), "tensor", None),
        P(("group", "expert", "seq"), None),
        P(("group", "expert", "seq"), None),
    )
    out_specs = P(("group", "expert", "seq"), "tensor")
    return jax.shard_map(body, mesh=mesh, in_specs=in_specs, out_specs=out_specs, check_vma=False)
```
